256 devices in a mesh: row: 8 (over y, z_lo), col: 32 (over x, z_hi, core).
Axes of the slice: x: 4, y: 4, z: 8 (z_hi: 4, z_lo: 2; z = z_hi * 2 + z_lo), core: 2. Of those that a mesh axis runs over, the one named last changes fastest.
Arguments:
- latent: bfloat16 [2, 512, 256, 320], P(None, 'row', 'col'), may hold values from -28 to 28
- timestep: int32 [2], replicated, may hold values from 0 to 999
- group_norm_gain: float32 [320], replicated, may hold values from 0.5 to 1.5
- group_norm_bias: float32 [320], replicated, may hold values from -0.5 to 0.5
- conv_w: bfloat16 [3, 3, 320, 320], replicated, may hold values from -0.109375 to 0.109375
- conv_b: float32 [320], replicated, may hold values from -0.5 to 0.5
- embed_in: bfloat16 [320, 1280], replicated, may hold values from -0.3125 to 0.3125
- embed_out: bfloat16 [1280, 1280], replicated, may hold values from -0.15625 to 0.15625
- time_w: bfloat16 [1280, 320], replicated, may hold values from -0.15625 to 0.15625
- cotangent: bfloat16 [2, 512, 256, 320], P(None, 'row', 'col'), may hold values from -6 to 6
Outputs:
- block_out: bfloat16 [2, 512, 256, 320], P(None, 'row', 'col')
- input_grad: float32 [2, 512, 256, 320], P(None, 'row', 'col')
- conv_w_grad: float32 [320, 3, 3, 320], P('row')
- gain_grad: float32 [320], replicated
- bias_grad: float32 [320], replicated
- conv_b_grad: float32 [320], replicated
- time_w_grad: float32 [1280, 320], replicated
The draws below stay inside these ranges and needn't reach their ends.
All inputs are finite; a program needn't handle non-finite values.
Results may differ from the reference program's by a relative error of at most 0.0055.
Values may be sent and summed in bfloat16 or wider, within the bound.
A program may use at most 128 MiB of HBM per device.

```python
import math
import jax
import jax.numpy as jnp
from jax import lax

C = 320
NORM_GROUPS = 32
TF = 320
TE = 1280
BATCH = 2
H = 512
W = 256


def draw_latent(key, part):
    base = jnp.clip(jax.random.normal(key, (BATCH, H, W, C), jnp.float32), -6.0, 6.0)
    row_count = jnp.arange(H, dtype=jnp.float32) / H
    column_count = jnp.arange(W, dtype=jnp.float32) / W
    spread = 3.0 ** (0.5 * row_count[:, None] + 0.5 * column_count[None, :])
    return (base * spread[None, :, :, None]).astype(jnp.bfloat16)


def level_of(key, dims, shards, least, largest):
    gain, own = 1.0, jax.random.fold_in(key, 6)
    for dim, parts in shards:
        steps = jnp.exp(jax.random.uniform(jax.random.fold_in(own, dim), (parts,), jnp.float32, least / len(shards), largest / len(shards)))
        gain = gain * jnp.repeat(steps, dims[dim] // parts).reshape([-1 if axis == dim else 1 for axis in range(len(dims))])
    return gain


def scatter_about(stream_key, extent, deviation, most, pieces=(), kind=jnp.bfloat16):
    drawn = deviation * jax.random.normal(stream_key, extent, jnp.float32)
    if pieces:
        drawn = drawn * level_of(stream_key, extent, pieces, -0.22, 0.18)
    return jnp.clip(drawn, -most, most).astype(kind)


def setup_inputs(seed: int = 0) -> dict:
    arg_keys = jax.random.split(jax.random.key(seed), 11)
    latent = draw_latent(jax.random.fold_in(arg_keys[10], 71), 0)
    timestep = jax.random.randint(arg_keys[1], (BATCH,), 0, 1000).astype(jnp.int32)
    group_norm_gain = jnp.clip(1.0 + 0.1 * jax.random.normal(arg_keys[2], (C,), jnp.float32), 0.5, 1.5)
    group_norm_bias = jnp.clip(jax.random.uniform(arg_keys[3], (C,), jnp.float32, -0.5, 0.5), -0.5, 0.5)
    conv_w = scatter_about(arg_keys[4], (3, 3, C, C), (9 * C) ** -0.5, 0.109375)
    conv_b = jnp.clip(jax.random.uniform(arg_keys[5], (C,), jnp.float32, -0.5, 0.5), -0.5, 0.5)
    embed_in = scatter_about(arg_keys[6], (TF, TE), TF ** -0.5, 0.3125)
    embed_out = scatter_about(arg_keys[7], (TE, TE), TE ** -0.5, 0.15625)
    time_w = scatter_about(arg_keys[8], (TE, C), TE ** -0.5, 0.15625)
    cotangent = scatter_about(arg_keys[9], (BATCH, H, W, C), 1.0, 6.0, ((1, 8), (2, 32)))
    return dict(latent=latent, timestep=timestep, group_norm_gain=group_norm_gain, group_norm_bias=group_norm_bias, conv_w=conv_w, conv_b=conv_b, embed_in=embed_in, embed_out=embed_out, time_w=time_w, cotangent=cotangent)


EPS = 1e-05

def embed(timestep, embed_in, embed_out):
    half = TF // 2
    freqs = jnp.exp(-math.log(10000.0) * jnp.arange(half, dtype=jnp.float32) / half)
    angles = timestep.astype(jnp.float32)[:, None] * freqs[None, :]
    sinus = jnp.concatenate([jnp.cos(angles), jnp.sin(angles)], axis=1).astype(jnp.bfloat16)
    first_hidden = jax.nn.silu(jnp.dot(sinus, embed_in, preferred_element_type=jnp.float32)).astype(jnp.bfloat16)
    return jax.nn.silu(jnp.dot(first_hidden, embed_out, preferred_element_type=jnp.float32)).astype(jnp.bfloat16)

def one_image(latent_img, temb_row, cot_img, group_norm_gain, group_norm_bias, conv_w, conv_b):
    row_count, column_count, channel_count = latent_img.shape
    channels_per_group = channel_count // NORM_GROUPS
    count = row_count * column_count * channels_per_group
    x = latent_img.astype(jnp.float32)
    grouped = x.reshape(row_count, column_count, NORM_GROUPS, channels_per_group)
    mean = lax.optimization_barrier(jnp.sum(grouped, axis=(0, 1, 3))) / count
    group_centered = grouped - mean[None, None, :, None]
    var = lax.optimization_barrier(jnp.sum(group_centered * group_centered, axis=(0, 1, 3))) / count
    inverse_deviation = lax.rsqrt(var + EPS)
    input_standardized = (group_centered * inverse_deviation[None, None, :, None]).reshape(row_count, column_count, channel_count)
    normed_output = input_standardized * group_norm_gain + group_norm_bias
    acts = jax.nn.silu(normed_output).astype(jnp.bfloat16)
    padded = jnp.pad(acts.astype(jnp.float32), ((1, 1), (1, 1), (0, 0)))
    weights = conv_w.astype(jnp.float32)
    conv = jnp.zeros((row_count, column_count, channel_count), jnp.float32)
    for kh in range(3):
        for kw in range(3):
            conv = conv + jnp.einsum('hwc,cd->hwd', padded[kh:kh + row_count, kw:kw + column_count], weights[kh, kw])
    block_out = (x + conv + conv_b + temb_row).astype(jnp.bfloat16)
    grad = cot_img.astype(jnp.float32)
    gpad = jnp.pad(grad, ((1, 1), (1, 1), (0, 0)))
    dacts = jnp.zeros((row_count, column_count, channel_count), jnp.float32)
    terms = []
    for kh in range(3):
        for kw in range(3):
            dacts = dacts + jnp.einsum('hwd,cd->hwc', gpad[2 - kh:2 - kh + row_count, 2 - kw:2 - kw + column_count], weights[kh, kw])
            terms.append(jnp.einsum('hwc,hwd->dc', padded[kh:kh + row_count, kw:kw + column_count], grad))
    wterm = jnp.stack(terms, axis=1).reshape(channel_count, 3, 3, channel_count)
    sig = jax.nn.sigmoid(normed_output)
    normed_gradient = dacts * sig * (1.0 + normed_output * (1.0 - sig))
    first = lax.optimization_barrier(jnp.sum(normed_gradient, axis=(0, 1)))
    second_moment = lax.optimization_barrier(jnp.sum(normed_gradient * input_standardized, axis=(0, 1)))
    gsum = lax.optimization_barrier(jnp.sum(grad, axis=(0, 1)))
    m_one = lax.optimization_barrier(jnp.sum((group_norm_gain * first).reshape(NORM_GROUPS, channels_per_group), axis=1)) / count
    m_two = lax.optimization_barrier(jnp.sum((group_norm_gain * second_moment).reshape(NORM_GROUPS, channels_per_group), axis=1)) / count
    dxhat = (normed_gradient * group_norm_gain).reshape(row_count, column_count, NORM_GROUPS, channels_per_group)
    input_grouped = input_standardized.reshape(row_count, column_count, NORM_GROUPS, channels_per_group)
    dx = inverse_deviation[None, None, :, None] * (dxhat - m_one[None, None, :, None] - input_grouped * m_two[None, None, :, None])
    input_grad = grad + dx.reshape(row_count, column_count, channel_count)
    return (block_out, input_grad, wterm, first, second_moment, gsum)

def reference(latent, timestep, group_norm_gain, group_norm_bias, conv_w, conv_b, embed_in, embed_out, time_w, cotangent):
    emb = embed(timestep, embed_in, embed_out)
    temb = jnp.dot(emb, time_w, preferred_element_type=jnp.float32)

    def step(items):
        return one_image(items[0], items[1], items[2], group_norm_gain, group_norm_bias, conv_w, conv_b)
    block_out, input_grad, wterm, first, second_moment, gsum = lax.map(step, (latent, temb, cotangent))
    scale = 1.0 / math.sqrt(BATCH * H * W)
    conv_w_grad = lax.optimization_barrier(jnp.sum(wterm, axis=0)) * scale
    gain_grad = lax.optimization_barrier(jnp.sum(second_moment, axis=0)) * scale
    bias_grad = lax.optimization_barrier(jnp.sum(first, axis=0)) * scale
    conv_b_grad = lax.optimization_barrier(jnp.sum(gsum, axis=0)) * scale
    time_w_grad = jnp.dot(emb.astype(jnp.float32).T, gsum) * scale
    return (block_out, input_grad, conv_w_grad, gain_grad, bias_grad, conv_b_grad, time_w_grad)
```

```python
import functools
import math

import jax
import jax.numpy as jnp
from jax import lax
from jax.experimental import pallas as pl
from jax.experimental.pallas import tpu as pltpu
from jax.sharding import Mesh
from jax.sharding import PartitionSpec as P

AXES = ("row_0", "row_1", "col_0", "col_1", "col_2")
ROW = ("row_0", "row_1")
COL = ("col_0", "col_1", "col_2")
EPS = 1e-05
GROUP = 10
C, CP = 320, 384
TE = 1280
B = 2
W = 8
TOP, OWN, PADROWS = 7, 8, 80
KP = 1024
f32, bf16 = jnp.float32, jnp.bfloat16
MESH = pl.DeviceIdType.MESH


def widen(v):
    return jnp.concatenate([v, jnp.zeros(v.shape[:-1] + (CP - C,), v.dtype)], axis=-1)


def dot(a, b):
    return jnp.dot(a, b, preferred_element_type=f32)


def dot_nt(a, b):
    return lax.dot_general(a, b, (((1,), (1,)), ((), ())), preferred_element_type=f32)


def pack_taps(put, v0, v1, v2):
    r = pltpu.roll(v1, 64, 1)
    put(0, 256, v0[:, 0:256])
    put(256, 128, v0[:, 256:384] + r[:, 0:128])
    put(384, 256, r[:, 128:384])
    put(640, 384, v2)


def group_sums(v):
    i = lax.broadcasted_iota(jnp.int32, (CP, CP), 0)
    j = lax.broadcasted_iota(jnp.int32, (CP, CP), 1)
    same = ((i * 6554) >> 16) == ((j * 6554) >> 16)
    ones = jnp.where(same & (i < C) & (j < C), 1.0, 0.0).astype(bf16)
    hi = v.astype(bf16)
    rest = v - hi.astype(f32)
    mid = rest.astype(bf16)
    low = (rest - mid.astype(f32)).astype(bf16)
    return dot(hi, ones) + dot(mid, ones) + dot(low, ones)


def kernel(
    sizes,
    H,
    ts_ref, gain_ref, bias_ref, cb_ref, lat_hbm, cot_hbm, cw_hbm, ein_hbm, eout_hbm, tw_hbm,
    bo_hbm, ig_hbm, cwg_ref, st_ref, gs_ref, emb_ref,
    in_v, cw_v, ein_v, eout_v, tw_v,
    row_in, col_out, col_in, cor_out, cor_in,
    lt, t80, gx, xx, wf, wt, da, co_v, gt, wg,
    sb1, r1, sb2, r2, sb3, r3, agb,
    a1, b1, a2, b2, ob, og,
    ld_sem, st_sem, halo_s, halo_r, ar_s, ar_r, s1_s, s1_r, s2_s, s2_r, s3_s, s3_r, ag_s, ag_r,
):
    Y, ZL, X, ZH, CO = sizes
    y, zl, x, zh, co = (lax.axis_index(a) for a in AXES)
    row, col = y * ZL + zl, (x * ZH + zh) * CO + co
    NR, NC = Y * ZL, X * ZH * CO
    NA, NB, NP, NZ = ZH * ZL * CO, X * Y, CO * X, ZH * ZL
    PL = 3 * KP // NP
    RB = 40 // NR
    RBZ = ZL * RB
    count = float(GROUP * H * NR * W * NC)
    scale = 1.0 / math.sqrt(B * H * NR * W * NC)

    def dev(y_=None, zl_=None, x_=None, zh_=None, co_=None):
        return {
            "row_0": y if y_ is None else y_,
            "row_1": zl if zl_ is None else zl_,
            "col_0": x if x_ is None else x_,
            "col_1": zh if zh_ is None else zh_,
            "col_2": co if co_ is None else co_,
        }

    def dev_at(r, c):
        return dev(r // ZL, lax.rem(r, ZL), c // (ZH * CO), lax.rem(c // CO, ZH), lax.rem(c, CO))

    ia, ib, iz, ip = (zh * ZL + zl) * CO + co, x * Y + y, zh * ZL + zl, co * X + x

    def peer_a(k):
        j = lax.rem(ia + k, NA)
        return j, dev(zl_=lax.rem(j // CO, ZL), zh_=j // (CO * ZL), co_=lax.rem(j, CO))

    def peer_b(k):
        j = lax.rem(ib + k, NB)
        return j, dev(x_=j // Y, y_=lax.rem(j, Y))

    def peer_z(k):
        j = lax.rem(iz + k, NZ)
        return j, dev(zl_=lax.rem(j, ZL), zh_=j // ZL)

    def peer_p(k):
        j = lax.rem(ip + k, NP)
        return j, dev(co_=j // X, x_=lax.rem(j, X))

    up, down = lax.rem(row + NR - 1, NR), lax.rem(row + 1, NR)
    left, right = lax.rem(col + NC - 1, NC), lax.rem(col + 1, NC)
    near = [dev_at(r, c) for r in (up, row, down) for c in (left, col, right) if not (r is row and c is col)]

    loads = [
        pltpu.make_async_copy(s, d, ld_sem.at[i])
        for i, (s, d) in enumerate(
            ((lat_hbm, in_v.at[0]), (cot_hbm, in_v.at[1]), (cw_hbm, cw_v), (ein_hbm, ein_v), (eout_hbm, eout_v), (tw_hbm, tw_v))
        )
    ]
    for cp in loads:
        cp.start()
    barrier = pltpu.get_barrier_semaphore()
    greeted = (
        [peer_a(k)[1] for k in range(1, NA)]
        + [peer_b(k)[1] for k in range(1, NB)]
        + [peer_p(k)[1] for k in range(1, NP)]
        + near
    )
    for d in greeted:
        pl.semaphore_signal(barrier, inc=1, device_id=d, device_id_type=MESH)

    sends = []

    def send(src, dst, s, r, d):
        cp = pltpu.make_async_remote_copy(src_ref=src, dst_ref=dst, send_sem=s, recv_sem=r, device_id=d, device_id_type=MESH)
        cp.start()
        sends.append(cp)
        return cp

    def zero(i, _):
        lt[i // (B * 10), lax.rem(i // 10, B), lax.rem(i, 10)] = jnp.zeros((PADROWS, CP), f32)
        return 0

    lax.fori_loop(0, 2 * B * 10, zero, 0)
    t80[...] = jnp.zeros_like(t80)

    def turn(arr, b, squares):
        def body(i, carry):
            h = pl.multiple_of(i * 8, 8)
            v = in_v[arr, b, pl.ds(h, 8)].astype(f32)
            lt[arr, b, 1:9, pl.ds(h + OWN, 8), 0:C] = jnp.transpose(v, (1, 0, 2))
            s = carry[0] + jnp.sum(v, axis=0)
            return (s, carry[1] + jnp.sum(v * v, axis=0)) if squares else (s,)

        z = jnp.zeros((W, C), f32)
        out = lax.fori_loop(0, H // 8, body, (z, z) if squares else (z,))
        return [widen(jnp.sum(o, axis=0, keepdims=True)) for o in out]

    loads[0].wait()
    sums = [turn(0, b, True) for b in range(B)]
    a1[ia] = jnp.concatenate([sums[0][0], sums[1][0], sums[0][1], sums[1][1], jnp.zeros((4, CP), f32)], axis=0)

    pl.semaphore_wait(barrier, len(greeted))

    def exchange(buf, own, sem, peers, n):
        for k in range(1, n):
            send(buf.at[own], buf.at[own], ar_s.at[sem, k], ar_r.at[sem, own], peers(k)[1])

    def gather_sum(buf, own, sem, peers, n):
        for k in range(1, n):
            j, d = peers(k)
            pltpu.make_async_remote_copy(
                src_ref=buf.at[j], dst_ref=buf.at[j], send_sem=ar_s.at[sem, k], recv_sem=ar_r.at[sem, j], device_id=d, device_id_type=MESH
            ).wait_recv()
        total = buf[0]
        for j in range(1, n):
            total = total + buf[j]
        return total

    exchange(a1, ia, 0, peer_a, NA)

    halos = []

    def halo(src, dst, i, d):
        halos.append(send(src, dst, halo_s.at[i], halo_r.at[i], d))

    loads[1].wait()
    for arr in range(2):
        halo(in_v.at[arr, :, H - 1], row_in.at[0, arr], arr, dev_at(down, col))
        halo(in_v.at[arr, :, 0], row_in.at[1, arr], 2 + arr, dev_at(up, col))
    gsum = [turn(1, b, False)[0] for b in range(B)]
    for arr in range(2):
        for b in range(B):
            col_out[0, arr, b] = lt[arr, b, 1, OWN : OWN + H, 0:C].astype(bf16)
            col_out[1, arr, b] = lt[arr, b, W, OWN : OWN + H, 0:C].astype(bf16)
            for r in range(2):
                for c in range(2):
                    i = OWN + (H - 1) * r
                    k = arr * B + b
                    cor_out[2 * r + c, k : k + 1, :] = lt[arr, b, 1 + (W - 1) * c, i : i + 1, :]
    for arr in range(2):
        halo(col_out.at[1, arr], col_in.at[0, arr], 4 + arr, dev_at(row, right))
        halo(col_out.at[0, arr], col_in.at[1, arr], 6 + arr, dev_at(row, left))
    for r in range(2):
        for c in range(2):
            halo(cor_out.at[2 * r + c], cor_in.at[2 * (1 - r) + 1 - c], 8 + 2 * r + c, dev_at((up, down)[r], (left, right)[c]))

    loads[2].wait()
    for kw in range(3):
        for kh in range(3):
            wf[kw, kh * C : (kh + 1) * C, :] = cw_v[kh, kw]
        wf[kw, 3 * C : KP, :] = jnp.zeros((KP - 3 * C, C), bf16)

        def turn_w(i, _):
            n = pl.multiple_of(i * 64, 64)
            v = [widen(cw_v[2 - kh, 2 - kw, pl.ds(n, 64), :].astype(f32)) for kh in range(3)]

            def put(at, wide, value):
                wt[kw, pl.ds(n, 64), at : at + wide] = value.astype(bf16)

            pack_taps(put, *v)
            return 0

        lax.fori_loop(0, C // 64, turn_w, 0)

    for cp in loads[3:]:
        cp.wait()
    lane = lax.broadcasted_iota(jnp.int32, (8, C), 1)
    step = jnp.where(lane < C // 2, lane, lane - C // 2).astype(f32)
    which = lax.broadcasted_iota(jnp.int32, (8, C), 0)
    time = jnp.where(which == 0, ts_ref[0].astype(f32), ts_ref[1].astype(f32))
    angle = time * jnp.exp(-math.log(10000.0) * step / (C // 2))
    sinus = jnp.where(lane < C // 2, jnp.cos(angle), jnp.sin(angle)).astype(bf16)
    hidden = jax.nn.silu(dot(sinus, ein_v[...])).astype(bf16)
    emb = jax.nn.silu(dot(hidden, eout_v[...])).astype(bf16)
    emb_ref[...] = emb.astype(f32)
    temb = dot(emb, tw_v[...]) + cb_ref[...].reshape(1, C)

    b1[ib] = gather_sum(a1, ia, 0, peer_a, NA)
    exchange(b1, ib, 1, peer_b, NB)

    for cp in halos:
        cp.wait_recv()
    keep = [
        jnp.where(row > 0, 1.0, 0.0),
        jnp.where(row < NR - 1, 1.0, 0.0),
        jnp.where(col > 0, 1.0, 0.0),
        jnp.where(col < NC - 1, 1.0, 0.0),
    ]
    for arr in range(2):
        for b in range(B):
            for side in range(2):
                at = OWN + H if side else TOP
                v = row_in[side, arr, b].astype(f32) * keep[side]
                for w in range(W):
                    lt[arr, b, w + 1, at : at + 1, 0:C] = v[w : w + 1]
                lt[arr, b, 9 * side, OWN : OWN + H, 0:C] = col_in[side, arr, b].astype(f32) * keep[2 + side]
                for c in range(2):
                    k = arr * B + b
                    lt[arr, b, 9 * c, at : at + 1, :] = cor_in[2 * side + c, k : k + 1, :] * keep[side] * keep[2 + c]

    def build_g(i, _):
        b, wq = i // 10, lax.rem(i, 10)

        def put(at, wide, value):
            gx[b, wq, :, at : at + wide] = value.astype(bf16)

        pack_taps(put, *(lt[1, b, wq, TOP + k : TOP + k + H, :] for k in range(3)))
        return 0

    lax.fori_loop(0, B * 10, build_g, 0)

    def dacts(i, _):
        b, w = i // 2, lax.rem(i, 2) * 4
        acc = dot_nt(gx[b, pl.ds(w, 4)].reshape(4 * H, KP), wt[0])
        for kw in range(1, 3):
            acc = acc + dot_nt(gx[b, pl.ds(w + kw, 4)].reshape(4 * H, KP), wt[kw])
        da[b, pl.ds(w, 4)] = widen(acc).reshape(4, H, CP)
        return 0

    lax.fori_loop(0, 2 * B, dacts, 0)
    part = max(128 // H, 1)
    for b in range(B):
        for k in range(W // part):
            v = lt[1, b, 1 + k * part : 1 + (k + 1) * part, OWN : OWN + H, :].reshape(part * H, CP)
            gt[b, :, k * part * H : (k + 1) * part * H] = jnp.transpose(v).astype(bf16)

    means = group_sums(gather_sum(b1, ib, 1, peer_b, NB)) / count
    gain, bias = widen(gain_ref[...].reshape(1, C)), widen(bias_ref[...].reshape(1, C))
    mean = [means[b : b + 1] for b in range(B)]
    rstd = [lax.rsqrt(means[B + b : B + b + 1] - mean[b] * mean[b] + EPS) for b in range(B)]
    line = lax.broadcasted_iota(jnp.int32, (PADROWS, CP), 0)
    rows_kept = jnp.where(line < OWN, keep[0], jnp.where(line < OWN + H, 1.0, keep[1]))

    def activate(b, wq, side_kept):
        mul = rstd[b] * gain
        normed = lt[0, b, wq] * mul + (bias - mean[b] * mul)
        sig = jax.nn.sigmoid(normed)
        t80[...] = normed * sig * (rows_kept * side_kept)

        def put(at, wide, value):
            xx[b, wq, :, at : at + wide] = value.astype(bf16)

        pack_taps(put, *(t80[TOP + k : TOP + k + H, :] for k in range(3)))
        return normed, sig

    halves = []
    for b in range(B):

        def own_column(w, carry):
            normed, sig = activate(b, w + 1, 1.0)
            normed, sig = normed[OWN : OWN + H], sig[OWN : OWN + H]
            dn = da[b, w] * sig * (1.0 + normed * (1.0 - sig))
            da[b, w] = dn
            xhat = (lt[0, b, w + 1, OWN : OWN + H, :] - mean[b]) * rstd[b]
            return (
                carry[0] + jnp.sum(dn.reshape(H // 8, 8, CP), axis=0),
                carry[1] + jnp.sum((dn * xhat).reshape(H // 8, 8, CP), axis=0),
            )

        z = jnp.zeros((8, CP), f32)
        halves.append([jnp.sum(o, axis=0, keepdims=True) for o in lax.fori_loop(0, W, own_column, (z, z))])
    a2[ia] = jnp.concatenate(
        [halves[0][0], halves[1][0], halves[0][1], halves[1][1], gsum[0], gsum[1], jnp.zeros((2, CP), f32)], axis=0
    )
    exchange(a2, ia, 2, peer_a, NA)
    for b in range(B):
        activate(b, 0, keep[2])
        activate(b, 9, keep[3])

    per = PL // 128
    for kw in range(3):
        for n in range(4):
            r = dot(gt[0, 0:C], xx[0, kw : kw + W, :, n * 256 : (n + 1) * 256].reshape(W * H, 256))
            r = r + dot(gt[1, 0:C], xx[1, kw : kw + W, :, n * 256 : (n + 1) * 256].reshape(W * H, 256))
            for t in range(2):
                tile = kw * 8 + n * 2 + t
                at = tile % per * 128
                wg[tile // per, :, at : at + 128] = r[:, t * 128 : (t + 1) * 128]

    def to_partner(i, _):
        sb1[i] = wg[(1 - co) * X + i].reshape(40, 8, PL).astype(bf16)
        return 0

    lax.fori_loop(0, X, to_partner, 0)
    first = send(sb1, r1, s1_s.at[0], s1_r.at[0], dev(co_=1 - co))

    def conv(b):
        def body(i, _):
            w = i * 4
            acc = dot(xx[b, pl.ds(w, 4)].reshape(4 * H, KP), wf[0])
            for kw in range(1, 3):
                acc = acc + dot(xx[b, pl.ds(w + kw, 4)].reshape(4 * H, KP), wf[kw])
            co_v[b, pl.ds(w, 4), :, 0:C] = acc.reshape(4, H, C)
            return 0

        lax.fori_loop(0, 2, body, 0)

        def emit(i, _):
            h = pl.multiple_of(i * 8, 8)
            v = co_v[b, :, pl.ds(h, 8), 0:C] + lt[0, b, 1:9, pl.ds(h + OWN, 8), 0:C] + temb[b : b + 1]
            ob[b, pl.ds(h, 8)] = jnp.transpose(v, (1, 0, 2)).astype(bf16)
            return 0

        lax.fori_loop(0, H // 8, emit, 0)
        out = pltpu.make_async_copy(ob.at[b], bo_hbm.at[b], st_sem.at[b])
        out.start()
        return out

    stores = [conv(0)]
    first.wait_recv()

    def halve(i, _):
        v = wg[co * X + i] + r1[i].astype(f32).reshape(C, PL)
        wg[co * X + i] = v
        sb2[i] = v.reshape(40, 8, PL).astype(bf16)
        return 0

    lax.fori_loop(0, X, halve, 0)
    second = []
    for dx in range(X):
        for dy in range(Y):
            if dx or dy:
                px, py = lax.rem(x + dx, X), lax.rem(y + dy, Y)
                k = dx * Y + dy
                second.append(send(sb2.at[px, pl.ds(py * RBZ, RBZ)], r2.at[k], s2_s.at[k], s2_r.at[k], dev(x_=px, y_=py)))
    b2[ib] = gather_sum(a2, ia, 2, peer_a, NA)
    exchange(b2, ib, 3, peer_b, NB)
    stores.append(conv(1))

    totals = gather_sum(b2, ib, 3, peer_b, NB)
    weights = jnp.concatenate([totals[0:4] * gain, jnp.zeros((4, CP), f32)], axis=0)
    groups = group_sums(weights) / count
    for b in range(B):
        m1, m2 = groups[b : b + 1, 0:C], groups[B + b : B + b + 1, 0:C]
        mb, rb = mean[b][:, 0:C], rstd[b][:, 0:C]

        def emit(i, _):
            h = pl.multiple_of(i * 8, 8)
            xv = lt[0, b, 1:9, pl.ds(h + OWN, 8), 0:C]
            gv = lt[1, b, 1:9, pl.ds(h + OWN, 8), 0:C]
            dn = da[b, :, pl.ds(h, 8), 0:C]
            v = gv + rb * (dn * gain[:, 0:C] - m1 - (xv - mb) * rb * m2)
            og[b, pl.ds(h, 8)] = jnp.transpose(v, (1, 0, 2))
            return 0

        lax.fori_loop(0, H // 8, emit, 0)
        out = pltpu.make_async_copy(og.at[b], ig_hbm.at[b], st_sem.at[B + b])
        out.start()
        stores.append(out)
    st_ref[...] = jnp.concatenate(
        [totals[2:3] + totals[3:4], totals[0:1] + totals[1:2], totals[4:5] + totals[5:6], jnp.zeros((5, CP), f32)], axis=0
    )[:, 0:C] * scale
    gs_ref[...] = jnp.concatenate([totals[4:6], jnp.zeros((6, CP), f32)], axis=0)[:, 0:C]

    for cp in second:
        cp.wait_recv()
    mine = wg[co * X + x, pl.ds(pl.multiple_of(y * (RBZ * 8), 8), RBZ * 8), :].reshape(RBZ, 8, PL)
    for k in range(1, NB):
        mine = mine + r2[k].astype(f32)
    sb3[...] = mine.astype(bf16)
    for k in range(1, NZ):
        j, d = peer_z(k)
        send(sb3.at[pl.ds(lax.rem(j, ZL) * RB, RB)], r3.at[iz], s3_s.at[k], s3_r.at[iz], d)
    r3[iz] = sb3[pl.ds(zl * RB, RB)]
    for k in range(1, NZ):
        j, d = peer_z(k)
        pltpu.make_async_remote_copy(
            src_ref=r3.at[j], dst_ref=r3.at[j], send_sem=s3_s.at[k], recv_sem=s3_r.at[j], device_id=d, device_id_type=MESH
        ).wait_recv()
    total = r3[0].astype(f32)
    for j in range(1, NZ):
        total = total + r3[j].astype(f32)
    agb[ip] = total.astype(bf16)
    for k in range(1, NP):
        send(agb.at[ip], agb.at[ip], ag_s.at[k], ag_r.at[ip], peer_p(k)[1])
    for k in range(1, NP):
        j, d = peer_p(k)
        pltpu.make_async_remote_copy(
            src_ref=agb.at[j], dst_ref=agb.at[j], send_sem=ag_s.at[k], recv_sem=ag_r.at[j], device_id=d, device_id_type=MESH
        ).wait_recv()
    for p in range(NP):
        cwg_ref[:, p * PL : (p + 1) * PL] = agb[p].astype(f32).reshape(RB * 8, PL) * scale
    for cp in sends:
        cp.wait_send()
    for cp in stores:
        cp.wait()


def step(sizes, latent, timestep, gain, bias, conv_w, conv_b, embed_in, embed_out, time_w, cotangent):
    Y, ZL, X, ZH, CO = sizes
    H = latent.shape[1]
    NA, NB, NP, NZ = ZH * ZL * CO, X * Y, CO * X, ZH * ZL
    PL = 3 * KP // NP
    RB = 40 // (Y * ZL)
    anyspace = pl.BlockSpec(memory_space=pl.ANY)
    vmem = pl.BlockSpec(memory_space=pltpu.VMEM)
    V, D = pltpu.VMEM, pltpu.SemaphoreType.DMA
    NG = max(NA, NB)
    bo, ig, cwg, st, gs, emb = pl.pallas_call(
        functools.partial(kernel, sizes, H),
        out_shape=(
            jax.ShapeDtypeStruct((B, H, W, C), bf16),
            jax.ShapeDtypeStruct((B, H, W, C), f32),
            jax.ShapeDtypeStruct((RB * 8, 3 * KP), f32),
            jax.ShapeDtypeStruct((8, C), f32),
            jax.ShapeDtypeStruct((8, C), f32),
            jax.ShapeDtypeStruct((8, TE), f32),
        ),
        in_specs=[pl.BlockSpec(memory_space=pltpu.SMEM)] + [vmem] * 3 + [anyspace] * 6,
        out_specs=(anyspace, anyspace, vmem, vmem, vmem, vmem),
        scratch_shapes=[
            V((2, B, H, W, C), bf16),
            V((3, 3, C, C), bf16),
            V((C, TE), bf16),
            V((TE, TE), bf16),
            V((TE, C), bf16),
            V((2, 2, B, W, C), bf16),
            V((2, 2, B, H, C), bf16),
            V((2, 2, B, H, C), bf16),
            V((4, 8, CP), f32),
            V((4, 8, CP), f32),
            V((2, B, 10, PADROWS, CP), f32),
            V((PADROWS, CP), f32),
            V((B, 10, H, KP), bf16),
            V((B, 10, H, KP), bf16),
            V((3, KP, C), bf16),
            V((3, C, KP), bf16),
            V((B, W, H, CP), f32),
            V((B, W, H, CP), f32),
            V((B, CP, W * H), bf16),
            V((NP, C, PL), f32),
            V((X, 40, 8, PL), bf16),
            V((X, 40, 8, PL), bf16),
            V((X, 40, 8, PL), bf16),
            V((NB, ZL * RB, 8, PL), bf16),
            V((ZL * RB, 8, PL), bf16),
            V((NZ, RB, 8, PL), bf16),
            V((NP, RB, 8, PL), bf16),
            V((NA, 8, CP), f32),
            V((NB, 8, CP), f32),
            V((NA, 8, CP), f32),
            V((NB, 8, CP), f32),
            V((B, H, W, C), bf16),
            V((B, H, W, C), f32),
            D((6,)),
            D((2 * B,)),
            D((12,)),
            D((12,)),
            D((4, NG)),
            D((4, NG)),
            D((1,)),
            D((1,)),
            D((NB,)),
            D((NB,)),
            D((NZ,)),
            D((NZ,)),
            D((NP,)),
            D((NP,)),
        ],
        compiler_params=pltpu.CompilerParams(collective_id=0, has_side_effects=True, vmem_limit_bytes=62 * 1024 * 1024),
        name="block",
    )(timestep, gain, bias, conv_b, latent, cotangent, conv_w, embed_in, embed_out, time_w)
    scale = 1.0 / math.sqrt(B * H * Y * ZL * W * X * ZH * CO)
    conv_w_grad = cwg.reshape(RB * 8, 3, KP)[:, :, : 3 * C].reshape(RB * 8, 3, 3, C).transpose(0, 2, 1, 3)
    time_w_grad = lax.dot_general(emb[0:B], gs[0:B], (((0,), (0,)), ((), ()))) * scale
    return bo, ig, conv_w_grad, st[0], st[1], st[2], time_w_grad


def build(finer):
    sizes = tuple(finer.shape[a] for a in AXES)
    image = P(None, ROW, COL, None)
    return jax.shard_map(
        functools.partial(step, sizes),
        mesh=finer,
        in_specs=(image, P(), P(), P(), P(), P(), P(), P(), P(), image),
        out_specs=(image, image, P(ROW, None, None, None), P(), P(), P(), P()),
        check_vma=False,
    )


def solution(mesh):
    return build(Mesh(mesh.devices.reshape(4, 2, 4, 4, 2), AXES))
```

```python
import functools
import math

import jax
import jax.numpy as jnp
from jax import lax
from jax.experimental import pallas as pl
from jax.experimental.pallas import tpu as pltpu
from jax.sharding import Mesh
from jax.sharding import PartitionSpec as P

AXES = ("row_0", "row_1", "col_0", "col_1", "col_2")
ROW = ("row_0", "row_1")
COL = ("col_0", "col_1", "col_2")
EPS = 1e-05
GROUP = 10
C, CP = 320, 384
TE = 1280
B = 2
W = 8
TOP, OWN, PADROWS = 7, 8, 80
KP = 1024
f32, bf16 = jnp.float32, jnp.bfloat16
MESH = pl.DeviceIdType.MESH


def widen(v):
    return jnp.concatenate([v, jnp.zeros(v.shape[:-1] + (CP - C,), v.dtype)], axis=-1)


def dot(a, b):
    return jnp.dot(a, b, preferred_element_type=f32)


def dot_nt(a, b):
    return lax.dot_general(a, b, (((1,), (1,)), ((), ())), preferred_element_type=f32)


def pack_taps(put, v0, v1, v2):
    r = pltpu.roll(v1, 64, 1)
    put(0, 256, v0[:, 0:256])
    put(256, 128, v0[:, 256:384] + r[:, 0:128])
    put(384, 256, r[:, 128:384])
    put(640, 384, v2)


def dot_exact(v, ones):
    hi = v.astype(bf16)
    rest = v - hi.astype(f32)
    mid = rest.astype(bf16)
    low = (rest - mid.astype(f32)).astype(bf16)
    return dot(hi, ones) + dot(mid, ones) + dot(low, ones)


def own_lanes():
    r = lax.broadcasted_iota(jnp.int32, (8, 128), 0)
    lane = lax.broadcasted_iota(jnp.int32, (8, 128), 1)
    return (lane >> 5) == r


def pack_groups(v):
    c = lax.broadcasted_iota(jnp.int32, (CP, 128), 0)
    lane = lax.broadcasted_iota(jnp.int32, (CP, 128), 1)
    ones = jnp.where((((c * 6554) >> 16) == (lane & 31)) & (c < C), 1.0, 0.0).astype(bf16)
    return jnp.sum(jnp.where(own_lanes(), dot_exact(v, ones), 0.0), axis=0, keepdims=True)


def spread_groups(t):
    lane = lax.broadcasted_iota(jnp.int32, (128, CP), 0)
    c = lax.broadcasted_iota(jnp.int32, (128, CP), 1)
    ones = jnp.where((((c * 6554) >> 16) == (lane & 31)) & (c < C), 1.0, 0.0).astype(bf16)
    return dot_exact(jnp.where(own_lanes(), jnp.broadcast_to(t, (8, 128)), 0.0), ones)


def stacked(rows, n):
    return jnp.concatenate(rows + [jnp.zeros((n - len(rows), CP), f32)], axis=0) if len(rows) < n else jnp.concatenate(rows, axis=0)


def kernel(
    sizes,
    H,
    ts_ref, gain_ref, bias_ref, cb_ref, lat_hbm, cot_hbm, cw_hbm, ein_hbm, eout_hbm, tw_hbm,
    bo_hbm, ig_hbm, cwg_ref, st_ref, gs_ref, emb_ref,
    in_v, cw_v, ein_v, eout_v, tw_v,
    row_in, col_out, col_in, cor_out, cor_in,
    lt, t80, gx, xx, wf, wt, da, co_v, gt, wg,
    sb1, r1, sb2, r2, sb3, r3, agb, wide, slope,
    a1, b1, a2, b2, a3, b3, ob, og,
    ld_sem, st_sem, halo_s, halo_r, ar_s, ar_r, s1_s, s1_r, s2_s, s2_r, s3_s, s3_r, ag_s, ag_r,
):
    Y, ZL, X, ZH, CO = sizes
    y, zl, x, zh, co = (lax.axis_index(a) for a in AXES)
    row, col = y * ZL + zl, (x * ZH + zh) * CO + co
    NR, NC = Y * ZL, X * ZH * CO
    NA, NB, NP, NZ = ZH * ZL * CO, X * Y, CO * X, ZH * ZL
    PL = 3 * KP // NP
    RB = 40 // NR
    RBZ = ZL * RB
    count = float(GROUP * H * NR * W * NC)
    scale = 1.0 / math.sqrt(B * H * NR * W * NC)

    def dev(y_=None, zl_=None, x_=None, zh_=None, co_=None):
        return {
            "row_0": y if y_ is None else y_,
            "row_1": zl if zl_ is None else zl_,
            "col_0": x if x_ is None else x_,
            "col_1": zh if zh_ is None else zh_,
            "col_2": co if co_ is None else co_,
        }

    def dev_at(r, c):
        return dev(r // ZL, lax.rem(r, ZL), c // (ZH * CO), lax.rem(c // CO, ZH), lax.rem(c, CO))

    ia, ib, iz, ip = (zh * ZL + zl) * CO + co, x * Y + y, zh * ZL + zl, co * X + x

    def peer_a(k):
        j = lax.rem(ia + k, NA)
        return j, dev(zl_=lax.rem(j // CO, ZL), zh_=j // (CO * ZL), co_=lax.rem(j, CO))

    def peer_b(k):
        j = lax.rem(ib + k, NB)
        return j, dev(x_=j // Y, y_=lax.rem(j, Y))

    def peer_z(k):
        j = lax.rem(iz + k, NZ)
        return j, dev(zl_=lax.rem(j, ZL), zh_=j // ZL)

    def peer_p(k):
        j = lax.rem(ip + k, NP)
        return j, dev(co_=j // X, x_=lax.rem(j, X))

    up, down = lax.rem(row + NR - 1, NR), lax.rem(row + 1, NR)
    left, right = lax.rem(col + NC - 1, NC), lax.rem(col + 1, NC)
    near = [dev_at(r, c) for r in (up, row, down) for c in (left, col, right) if not (r is row and c is col)]

    loads = [
        pltpu.make_async_copy(s, d, ld_sem.at[i])
        for i, (s, d) in enumerate(
            ((lat_hbm, in_v.at[0]), (cot_hbm, in_v.at[1]), (cw_hbm, cw_v), (ein_hbm, ein_v), (eout_hbm, eout_v), (tw_hbm, tw_v))
        )
    ]
    for cp in loads:
        cp.start()
    barrier = pltpu.get_barrier_semaphore()
    greeted = (
        [peer_a(k)[1] for k in range(1, NA)]
        + [peer_b(k)[1] for k in range(1, NB)]
        + [peer_p(k)[1] for k in range(1, NP)]
        + near
    )
    for d in greeted:
        pl.semaphore_signal(barrier, inc=1, device_id=d, device_id_type=MESH)

    sends = []

    def send(src, dst, s, r, d):
        cp = pltpu.make_async_remote_copy(src_ref=src, dst_ref=dst, send_sem=s, recv_sem=r, device_id=d, device_id_type=MESH)
        cp.start()
        sends.append(cp)
        return cp

    def zero(i, _):
        lt[i // (B * 10), lax.rem(i // 10, B), lax.rem(i, 10)] = jnp.zeros((PADROWS, CP), f32)
        return 0

    lax.fori_loop(0, 2 * B * 10, zero, 0)
    t80[...] = jnp.zeros_like(t80)

    def turn(arr, b, squares):
        def body(i, carry):
            h = pl.multiple_of(i * 8, 8)
            v = in_v[arr, b, pl.ds(h, 8)].astype(f32)
            lt[arr, b, 1:9, pl.ds(h + OWN, 8), 0:C] = jnp.transpose(v, (1, 0, 2))
            s = carry[0] + jnp.sum(v, axis=0)
            return (s, carry[1] + jnp.sum(v * v, axis=0)) if squares else (s,)

        z = jnp.zeros((W, C), f32)
        out = lax.fori_loop(0, H // 8, body, (z, z) if squares else (z,))
        return [widen(jnp.sum(o, axis=0, keepdims=True)) for o in out]

    loads[0].wait()
    sums = [turn(0, b, True) for b in range(B)]
    a1[ia] = pack_groups(stacked([sums[0][0], sums[1][0], sums[0][1], sums[1][1]], 8))

    pl.semaphore_wait(barrier, len(greeted))

    def exchange(buf, own, sem, peers, n):
        for k in range(1, n):
            send(buf.at[own], buf.at[own], ar_s.at[sem, k], ar_r.at[sem, own], peers(k)[1])

    def gather_sum(buf, own, sem, peers, n):
        for k in range(1, n):
            j, d = peers(k)
            pltpu.make_async_remote_copy(
                src_ref=buf.at[j], dst_ref=buf.at[j], send_sem=ar_s.at[sem, k], recv_sem=ar_r.at[sem, j], device_id=d, device_id_type=MESH
            ).wait_recv()
        total = buf[0]
        for j in range(1, n):
            total = total + buf[j]
        return total

    exchange(a1, ia, 0, peer_a, NA)

    halos = []

    def halo(src, dst, i, d):
        halos.append(send(src, dst, halo_s.at[i], halo_r.at[i], d))

    loads[1].wait()
    for arr in range(2):
        halo(in_v.at[arr, :, H - 1], row_in.at[0, arr], arr, dev_at(down, col))
        halo(in_v.at[arr, :, 0], row_in.at[1, arr], 2 + arr, dev_at(up, col))
    gsum = [turn(1, b, False)[0] for b in range(B)]
    for arr in range(2):
        for b in range(B):
            col_out[0, arr, b] = lt[arr, b, 1, OWN : OWN + H, 0:C].astype(bf16)
            col_out[1, arr, b] = lt[arr, b, W, OWN : OWN + H, 0:C].astype(bf16)
            for r in range(2):
                for c in range(2):
                    i = OWN + (H - 1) * r
                    k = arr * B + b
                    cor_out[2 * r + c, k : k + 1, :] = lt[arr, b, 1 + (W - 1) * c, i : i + 1, :]
    for arr in range(2):
        halo(col_out.at[1, arr], col_in.at[0, arr], 4 + arr, dev_at(row, right))
        halo(col_out.at[0, arr], col_in.at[1, arr], 6 + arr, dev_at(row, left))
    for r in range(2):
        for c in range(2):
            halo(cor_out.at[2 * r + c], cor_in.at[2 * (1 - r) + 1 - c], 8 + 2 * r + c, dev_at((up, down)[r], (left, right)[c]))

    loads[2].wait()
    for kw in range(3):
        for kh in range(3):
            wf[kw, kh * C : (kh + 1) * C, :] = cw_v[kh, kw]
        wf[kw, 3 * C : KP, :] = jnp.zeros((KP - 3 * C, C), bf16)

        def turn_w(i, _):
            n = pl.multiple_of(i * 64, 64)
            v = [widen(cw_v[2 - kh, 2 - kw, pl.ds(n, 64), :].astype(f32)) for kh in range(3)]

            def put(at, wide, value):
                wt[kw, pl.ds(n, 64), at : at + wide] = value.astype(bf16)

            pack_taps(put, *v)
            return 0

        lax.fori_loop(0, C // 64, turn_w, 0)
    part = max(128 // H, 1)
    for b in range(B):
        for k in range(W // part):
            v = lt[1, b, 1 + k * part : 1 + (k + 1) * part, OWN : OWN + H, :].reshape(part * H, CP)
            gt[b, :, k * part * H : (k + 1) * part * H] = jnp.transpose(v).astype(bf16)

    b1[ib] = gather_sum(a1, ia, 0, peer_a, NA)
    exchange(b1, ib, 1, peer_b, NB)

    for cp in loads[3:]:
        cp.wait()
    lane = lax.broadcasted_iota(jnp.int32, (8, C), 1)
    step = jnp.where(lane < C // 2, lane, lane - C // 2).astype(f32)
    which = lax.broadcasted_iota(jnp.int32, (8, C), 0)
    time = jnp.where(which == 0, ts_ref[0].astype(f32), ts_ref[1].astype(f32))
    angle = time * jnp.exp(-math.log(10000.0) * step / (C // 2))
    sinus = jnp.where(lane < C // 2, jnp.cos(angle), jnp.sin(angle)).astype(bf16)
    hidden = jax.nn.silu(dot(sinus, ein_v[...])).astype(bf16)
    emb = jax.nn.silu(dot(hidden, eout_v[...])).astype(bf16)
    emb_ref[...] = emb.astype(f32)
    temb = dot_nt(emb, tw_v[...]) + cb_ref[...].reshape(1, C)

    for cp in halos:
        cp.wait_recv()
    keep = [
        jnp.where(row > 0, 1.0, 0.0),
        jnp.where(row < NR - 1, 1.0, 0.0),
        jnp.where(col > 0, 1.0, 0.0),
        jnp.where(col < NC - 1, 1.0, 0.0),
    ]
    for arr in range(2):
        for b in range(B):
            for side in range(2):
                at = OWN + H if side else TOP
                v = row_in[side, arr, b].astype(f32) * keep[side]
                for w in range(W):
                    lt[arr, b, w + 1, at : at + 1, 0:C] = v[w : w + 1]
                lt[arr, b, 9 * side, OWN : OWN + H, 0:C] = col_in[side, arr, b].astype(f32) * keep[2 + side]
                for c in range(2):
                    k = arr * B + b
                    lt[arr, b, 9 * c, at : at + 1, :] = cor_in[2 * side + c, k : k + 1, :] * keep[side] * keep[2 + c]

    def build_g(i, _):
        for b in range(B):
            for n in range(2):
                wq = i * 2 + n

                def put(at, wide, value):
                    gx[b, wq, :, at : at + wide] = value.astype(bf16)

                pack_taps(put, *(lt[1, b, wq, TOP + k : TOP + k + H, :] for k in range(3)))
        return 0

    lax.fori_loop(0, 5, build_g, 0)

    means = spread_groups(gather_sum(b1, ib, 1, peer_b, NB)) / count
    gain, bias = widen(gain_ref[...].reshape(1, C)), widen(bias_ref[...].reshape(1, C))
    mean = [means[b : b + 1] for b in range(B)]
    rstd = [lax.rsqrt(means[B + b : B + b + 1] - mean[b] * mean[b] + EPS) for b in range(B)]
    line = lax.broadcasted_iota(jnp.int32, (PADROWS, CP), 0)
    rows_kept = jnp.where(line < OWN, keep[0], jnp.where(line < OWN + H, 1.0, keep[1]))

    def activate(b, wq, side_kept, n):
        mul = rstd[b] * gain
        normed = lt[0, b, wq] * mul + (bias - mean[b] * mul)
        sig = jax.nn.sigmoid(normed)
        t80[n] = normed * sig * (rows_kept * side_kept)

        def put(at, wide, value):
            xx[b, wq, :, at : at + wide] = value.astype(bf16)

        pack_taps(put, *(t80[n, TOP + k : TOP + k + H, :] for k in range(3)))
        return normed, sig

    def own_columns(i, _):
        for b in range(B):
            for n in range(2):
                w = i * 2 + n
                normed, sig = activate(b, w + 1, 1.0, b * 2 + n)
                normed, sig = normed[OWN : OWN + H], sig[OWN : OWN + H]
                slope[b, w] = sig * (1.0 + normed * (1.0 - sig))
        return 0

    lax.fori_loop(0, W // 2, own_columns, 0)
    for b in range(B):
        activate(b, 0, keep[2], b * 2)
        activate(b, 9, keep[3], b * 2 + 1)

    per = PL // 128
    for kw in range(3):
        for n in range(4):
            r = dot(gt[0, 0:C], xx[0, kw : kw + W, :, n * 256 : (n + 1) * 256].reshape(W * H, 256))
            r = r + dot(gt[1, 0:C], xx[1, kw : kw + W, :, n * 256 : (n + 1) * 256].reshape(W * H, 256))
            for t in range(2):
                tile = kw * 8 + n * 2 + t
                at = tile % per * 128
                wg[tile // per, :, at : at + 128] = r[:, t * 128 : (t + 1) * 128]

    def to_partner(i, _):
        sb1[i] = wg[(1 - co) * X + i].reshape(40, 8, PL).astype(bf16)
        return 0

    lax.fori_loop(0, X, to_partner, 0)
    first = send(sb1, r1, s1_s.at[0], s1_r.at[0], dev(co_=1 - co))

    def dacts(i, _):
        b, w = i // 2, lax.rem(i, 2) * 4
        acc = dot_nt(gx[b, pl.ds(w, 4)].reshape(4 * H, KP), wt[0])
        for kw in range(1, 3):
            acc = acc + dot_nt(gx[b, pl.ds(w + kw, 4)].reshape(4 * H, KP), wt[kw])
        da[b, pl.ds(w, 4)] = widen(acc).reshape(4, H, CP)
        return 0

    def conv(b):
        def body(i, _):
            w = i * 4
            acc = dot(xx[b, pl.ds(w, 4)].reshape(4 * H, KP), wf[0])
            for kw in range(1, 3):
                acc = acc + dot(xx[b, pl.ds(w + kw, 4)].reshape(4 * H, KP), wf[kw])
            co_v[b, pl.ds(w, 4), :, 0:C] = acc.reshape(4, H, C)
            return 0

        lax.fori_loop(0, 2, body, 0)

        def emit(i, _):
            h = pl.multiple_of(i * 8, 8)
            v = co_v[b, :, pl.ds(h, 8), 0:C] + lt[0, b, 1:9, pl.ds(h + OWN, 8), 0:C] + temb[b : b + 1]
            ob[b, pl.ds(h, 8)] = jnp.transpose(v, (1, 0, 2)).astype(bf16)
            return 0

        lax.fori_loop(0, H // 8, emit, 0)
        out = pltpu.make_async_copy(ob.at[b], bo_hbm.at[b], st_sem.at[b])
        out.start()
        return out

    lax.fori_loop(0, B, dacts, 0)
    first.wait_recv()

    def halve(i, _):
        v = wg[co * X + i] + r1[i].astype(f32).reshape(C, PL)
        wg[co * X + i] = v
        sb2[i] = v.reshape(40, 8, PL).astype(bf16)
        return 0

    lax.fori_loop(0, X, halve, 0)
    T = 3
    CH = PL // T
    second = [[] for _ in range(T)]
    for t in range(T):
        lanes = pl.ds(t * CH, CH)
        for dx in range(X):
            for dy in range(Y):
                if dx or dy:
                    px, py = lax.rem(x + dx, X), lax.rem(y + dy, Y)
                    k = dx * Y + dy
                    second[t].append(
                        send(
                            sb2.at[px, pl.ds(py * RBZ, RBZ), :, lanes], r2.at[k, :, :, lanes],
                            s2_s.at[t, k], s2_r.at[t, k], dev(x_=px, y_=py),
                        )
                    )
    lax.fori_loop(B, 2 * B, dacts, 0)
    halves = []
    for b in range(B):

        def own_column(i, carry):
            s1, s2 = carry
            for n in range(2):
                w = i * 2 + n
                dn = da[b, w] * slope[b, w]
                da[b, w] = dn
                xhat = (lt[0, b, w + 1, OWN : OWN + H, :] - mean[b]) * rstd[b]
                s1 = s1 + jnp.sum(dn.reshape(H // 8, 8, CP), axis=0)
                s2 = s2 + jnp.sum((dn * xhat).reshape(H // 8, 8, CP), axis=0)
            return s1, s2

        z = jnp.zeros((8, CP), f32)
        halves.append([jnp.sum(o, axis=0, keepdims=True) for o in lax.fori_loop(0, W // 2, own_column, (z, z))])
    a2[ia] = pack_groups(stacked([halves[0][0] * gain, halves[1][0] * gain, halves[0][1] * gain, halves[1][1] * gain], 8))
    exchange(a2, ia, 2, peer_a, NA)
    a3[ia] = stacked([halves[0][0] + halves[1][0], halves[0][1] + halves[1][1], gsum[0], gsum[1]], 4)
    exchange(a3, ia, 4, peer_a, NA)
    stores = [conv(0)]
    b2[ib] = gather_sum(a2, ia, 2, peer_a, NA)
    exchange(b2, ib, 3, peer_b, NB)
    b3[ib] = gather_sum(a3, ia, 4, peer_a, NA)
    exchange(b3, ib, 5, peer_b, NB)

    def over_z(t):
        lanes = slice(t * CH, (t + 1) * CH)
        for cp in second[t]:
            cp.wait_recv()
        mine = wg[co * X + x, pl.ds(pl.multiple_of(y * (RBZ * 8), 8), RBZ * 8), lanes].reshape(RBZ, 8, CH)
        for k in range(1, NB):
            mine = mine + r2[k, :, :, lanes].astype(f32)
        sb3[:, :, lanes] = mine.astype(bf16)
        for k in range(1, NZ):
            j, d = peer_z(k)
            send(
                sb3.at[pl.ds(lax.rem(j, ZL) * RB, RB), :, lanes], r3.at[iz, :, :, lanes], s3_s.at[t, k], s3_r.at[t, iz], d
            )
        r3[iz, :, :, lanes] = sb3[pl.ds(zl * RB, RB), :, lanes]

    def to_holders(t):
        lanes = slice(t * CH, (t + 1) * CH)
        for k in range(1, NZ):
            j, d = peer_z(k)
            part = r3.at[j, :, :, lanes]
            pltpu.make_async_remote_copy(
                src_ref=part, dst_ref=part, send_sem=s3_s.at[t, k], recv_sem=s3_r.at[t, j], device_id=d, device_id_type=MESH
            ).wait_recv()
        total = r3[0, :, :, lanes].astype(f32)
        for j in range(1, NZ):
            total = total + r3[j, :, :, lanes].astype(f32)
        agb[ip, :, :, lanes] = total.astype(bf16)
        for k in range(1, NP):
            part = agb.at[ip, :, :, lanes]
            send(part, part, ag_s.at[t, k], ag_r.at[t, ip], peer_p(k)[1])

    over_z(0)
    stores.append(conv(1))
    over_z(1)
    over_z(2)
    to_holders(0)
    to_holders(1)

    groups = spread_groups(gather_sum(b2, ib, 3, peer_b, NB)) / count
    totals = gather_sum(b3, ib, 5, peer_b, NB)
    for b in range(B):
        m1, m2 = groups[b : b + 1, 0:C], groups[B + b : B + b + 1, 0:C]
        mb, rb = mean[b][:, 0:C], rstd[b][:, 0:C]

        def emit(i, _):
            h = pl.multiple_of(i * 8, 8)
            xv = lt[0, b, 1:9, pl.ds(h + OWN, 8), 0:C]
            gv = lt[1, b, 1:9, pl.ds(h + OWN, 8), 0:C]
            dn = da[b, :, pl.ds(h, 8), 0:C]
            v = gv + rb * (dn * gain[:, 0:C] - m1 - (xv - mb) * rb * m2)
            og[b, pl.ds(h, 8)] = jnp.transpose(v, (1, 0, 2))
            return 0

        lax.fori_loop(0, H // 8, emit, 0)
        out = pltpu.make_async_copy(og.at[b], ig_hbm.at[b], st_sem.at[B + b])
        out.start()
        stores.append(out)
    st_ref[...] = (stacked([totals[1:2], totals[0:1], totals[2:3] + totals[3:4]], 8) * scale)[:, 0:C]
    gs_ref[...] = stacked([totals[2:3], totals[3:4]], 8)[:, 0:C]

    to_holders(2)
    for t in range(T):
        lanes = slice(t * CH, (t + 1) * CH)
        for k in range(1, NP):
            j, d = peer_p(k)
            part = agb.at[j, :, :, lanes]
            pltpu.make_async_remote_copy(
                src_ref=part, dst_ref=part, send_sem=ag_s.at[t, k], recv_sem=ag_r.at[t, j], device_id=d, device_id_type=MESH
            ).wait_recv()
    for p in range(NP):
        wide[:, p * PL : (p + 1) * PL] = agb[p].astype(f32).reshape(RB * 8, PL) * scale
    for kw in range(3):
        at = kw * KP
        cwg_ref[0, kw] = wide[:, at : at + C]
        cwg_ref[1, kw] = pltpu.roll(wide[:, at + 256 : at + 640], CP - 64, 1)[:, 0:C]
        cwg_ref[2, kw] = wide[:, at + 2 * C : at + 3 * C]
    for cp in sends:
        cp.wait_send()
    for cp in stores:
        cp.wait()


def step(sizes, latent, timestep, gain, bias, conv_w, conv_b, embed_in, embed_out, time_w, cotangent):
    Y, ZL, X, ZH, CO = sizes
    H = latent.shape[1]
    NA, NB, NP, NZ = ZH * ZL * CO, X * Y, CO * X, ZH * ZL
    PL = 3 * KP // NP
    RB = 40 // (Y * ZL)
    anyspace = pl.BlockSpec(memory_space=pl.ANY)
    vmem = pl.BlockSpec(memory_space=pltpu.VMEM)
    V, D = pltpu.VMEM, pltpu.SemaphoreType.DMA
    NG = max(NA, NB)
    bo, ig, cwg, st, gs, emb = pl.pallas_call(
        functools.partial(kernel, sizes, H),
        out_shape=(
            jax.ShapeDtypeStruct((B, H, W, C), bf16),
            jax.ShapeDtypeStruct((B, H, W, C), f32),
            jax.ShapeDtypeStruct((3, 3, RB * 8, C), f32),
            jax.ShapeDtypeStruct((8, C), f32),
            jax.ShapeDtypeStruct((8, C), f32),
            jax.ShapeDtypeStruct((8, TE), f32),
        ),
        in_specs=[pl.BlockSpec(memory_space=pltpu.SMEM)] + [vmem] * 3 + [anyspace] * 6,
        out_specs=(anyspace, anyspace, vmem, vmem, vmem, vmem),
        scratch_shapes=[
            V((2, B, H, W, C), bf16),
            V((3, 3, C, C), bf16),
            V((C, TE), bf16),
            V((TE, TE), bf16),
            V((C, TE), bf16),
            V((2, 2, B, W, C), bf16),
            V((2, 2, B, H, C), bf16),
            V((2, 2, B, H, C), bf16),
            V((4, 8, CP), f32),
            V((4, 8, CP), f32),
            V((2, B, 10, PADROWS, CP), f32),
            V((4, PADROWS, CP), f32),
            V((B, 10, H, KP), bf16),
            V((B, 10, H, KP), bf16),
            V((3, KP, C), bf16),
            V((3, C, KP), bf16),
            V((B, W, H, CP), f32),
            V((B, W, H, CP), f32),
            V((B, CP, W * H), bf16),
            V((NP, C, PL), f32),
            V((X, 40, 8, PL), bf16),
            V((X, 40, 8, PL), bf16),
            V((X, 40, 8, PL), bf16),
            V((NB, ZL * RB, 8, PL), bf16),
            V((ZL * RB, 8, PL), bf16),
            V((NZ, RB, 8, PL), bf16),
            V((NP, RB, 8, PL), bf16),
            V((RB * 8, 3 * KP), f32),
            V((B, W, H, CP), f32),
            V((NA, 1, 128), f32),
            V((NB, 1, 128), f32),
            V((NA, 1, 128), f32),
            V((NB, 1, 128), f32),
            V((NA, 4, CP), f32),
            V((NB, 4, CP), f32),
            V((B, H, W, C), bf16),
            V((B, H, W, C), f32),
            D((6,)),
            D((2 * B,)),
            D((12,)),
            D((12,)),
            D((6, NG)),
            D((6, NG)),
            D((1,)),
            D((1,)),
            D((3, NB)),
            D((3, NB)),
            D((3, NZ)),
            D((3, NZ)),
            D((3, NP)),
            D((3, NP)),
        ],
        compiler_params=pltpu.CompilerParams(collective_id=0, has_side_effects=True, vmem_limit_bytes=62 * 1024 * 1024),
        name="block",
    )(timestep, gain, bias, conv_b, latent, cotangent, conv_w, embed_in, embed_out, time_w.T)
    scale = 1.0 / math.sqrt(B * H * Y * ZL * W * X * ZH * CO)
    conv_w_grad = cwg.transpose(2, 0, 1, 3)
    time_w_grad = lax.dot_general(emb[0:B], gs[0:B], (((0,), (0,)), ((), ()))) * scale
    return bo, ig, conv_w_grad, st[0], st[1], st[2], time_w_grad


def build(finer):
    sizes = tuple(finer.shape[a] for a in AXES)
    image = P(None, ROW, COL, None)
    return jax.shard_map(
        functools.partial(step, sizes),
        mesh=finer,
        in_specs=(image, P(), P(), P(), P(), P(), P(), P(), P(), image),
        out_specs=(image, image, P(ROW, None, None, None), P(), P(), P(), P()),
        check_vma=False,
    )


def solution(mesh):
    return build(Mesh(mesh.devices.reshape(4, 2, 4, 4, 2), AXES))
```

```python
import functools
import math

import jax
import jax.numpy as jnp
from jax import lax
from jax.experimental import pallas as pl
from jax.experimental.pallas import tpu as pltpu
from jax.sharding import Mesh
from jax.sharding import PartitionSpec as P

AXES = ("row_0", "row_1", "col_0", "col_1", "col_2")
ROW = ("row_0", "row_1")
COL = ("col_0", "col_1", "col_2")
EPS = 1e-05
GROUP = 10
C, CP = 320, 384
TE = 1280
B = 2
W = 8
TOP, OWN, PADROWS = 7, 8, 80
KP = 1024
f32, bf16 = jnp.float32, jnp.bfloat16
MESH = pl.DeviceIdType.MESH
HELD = pltpu.VMEM
LIMIT = 50 * 1024 * 1024


def widen(v):
    return jnp.concatenate([v, jnp.zeros(v.shape[:-1] + (CP - C,), v.dtype)], axis=-1)


def dot(a, b):
    return jnp.dot(a, b, preferred_element_type=f32)


def dot_nt(a, b):
    return lax.dot_general(a, b, (((1,), (1,)), ((), ())), preferred_element_type=f32)


def pack_taps(put, v0, v1, v2):
    r = pltpu.roll(v1, 64, 1)
    put(0, 256, v0[:, 0:256])
    put(256, 128, v0[:, 256:384] + r[:, 0:128])
    put(384, 256, r[:, 128:384])
    put(640, 384, v2)


def dot_exact(v, ones):
    hi = v.astype(bf16)
    rest = v - hi.astype(f32)
    mid = rest.astype(bf16)
    low = (rest - mid.astype(f32)).astype(bf16)
    return dot(hi, ones) + dot(mid, ones) + dot(low, ones)


def own_lanes():
    r = lax.broadcasted_iota(jnp.int32, (8, 128), 0)
    lane = lax.broadcasted_iota(jnp.int32, (8, 128), 1)
    return (lane >> 5) == r


def pack_groups(v):
    c = lax.broadcasted_iota(jnp.int32, (CP, 128), 0)
    lane = lax.broadcasted_iota(jnp.int32, (CP, 128), 1)
    ones = jnp.where((((c * 6554) >> 16) == (lane & 31)) & (c < C), 1.0, 0.0).astype(bf16)
    return jnp.sum(jnp.where(own_lanes(), dot_exact(v, ones), 0.0), axis=0, keepdims=True)


def spread_groups(t):
    lane = lax.broadcasted_iota(jnp.int32, (128, CP), 0)
    c = lax.broadcasted_iota(jnp.int32, (128, CP), 1)
    ones = jnp.where((((c * 6554) >> 16) == (lane & 31)) & (c < C), 1.0, 0.0).astype(bf16)
    return dot_exact(jnp.where(own_lanes(), jnp.broadcast_to(t, (8, 128)), 0.0), ones)


def stacked(rows, n):
    return jnp.concatenate(rows + [jnp.zeros((n - len(rows), CP), f32)], axis=0) if len(rows) < n else jnp.concatenate(rows, axis=0)


def kernel(
    sizes,
    H,
    ts_hbm, gain_hbm, bias_hbm, cb_hbm, lat_hbm, cot_hbm, cw_hbm, ein_hbm, eout_hbm, tw_hbm,
    ob, og, cwg_ref, st_ref, twg_ref,
    ts_ref, gain_ref, bias_ref, cb_ref,
    in_v, cw_v, ein_v, eout_v, tw_v,
    row_in, col_out, col_in, cor_out, cor_in,
    lt, t80, gx, xx, wf, wt, da, co_v, gt, wg, wg2, wg3, wg4,
    sb1, r1, sb2, rx, ry, ux, uy, vx, vy, sb3, r3, agb, slope,
    a1, b1, a2, b2, a3, b3,
    ld_sem, halo_s, halo_r, ar_s, ar_r, s1_s, s1_r, x_s, x_r, y_s, y_r, x2_s, x2_r, y2_s, y2_r, s3_s, s3_r, ag_s, ag_r,
):
    Y, ZL, X, ZH, CO = sizes
    y, zl, x, zh, co = (lax.axis_index(a) for a in AXES)
    row, col = y * ZL + zl, (x * ZH + zh) * CO + co
    NR, NC = Y * ZL, X * ZH * CO
    NA, NB, NP, NZ = ZH * ZL * CO, X * Y, CO * X, ZH * ZL
    HALF = KP // CO
    CH = HALF // X
    RB = 40 // NR
    count = float(GROUP * H * NR * W * NC)
    scale = 1.0 / math.sqrt(B * H * NR * W * NC)

    def dev(y_=None, zl_=None, x_=None, zh_=None, co_=None):
        return {
            "row_0": y if y_ is None else y_,
            "row_1": zl if zl_ is None else zl_,
            "col_0": x if x_ is None else x_,
            "col_1": zh if zh_ is None else zh_,
            "col_2": co if co_ is None else co_,
        }

    def dev_at(r, c):
        return dev(r // ZL, lax.rem(r, ZL), c // (ZH * CO), lax.rem(c // CO, ZH), lax.rem(c, CO))

    ia, ib, iz, ip = (zh * ZL + zl) * CO + co, x * Y + y, zh * ZL + zl, co * X + x

    def peer_a(k):
        j = lax.rem(ia + k, NA)
        return j, dev(zl_=lax.rem(j // CO, ZL), zh_=j // (CO * ZL), co_=lax.rem(j, CO))

    def peer_b(k):
        j = lax.rem(ib + k, NB)
        return j, dev(x_=j // Y, y_=lax.rem(j, Y))

    def peer_z(k):
        j = lax.rem(iz + k, NZ)
        return j, dev(zl_=lax.rem(j, ZL), zh_=j // ZL)

    def peer_p(k):
        j = lax.rem(ip + k, NP)
        return j, dev(co_=j // X, x_=lax.rem(j, X))

    up, down = lax.rem(row + NR - 1, NR), lax.rem(row + 1, NR)
    left, right = lax.rem(col + NC - 1, NC), lax.rem(col + 1, NC)
    near = [dev_at(r, c) for r in (up, row, down) for c in (left, col, right) if not (r is row and c is col)]

    pairs = (
        (lat_hbm, in_v.at[0]), (ts_hbm, ts_ref), (gain_hbm, gain_ref), (bias_hbm, bias_ref), (cb_hbm, cb_ref),
        (cot_hbm, in_v.at[1]), (cw_hbm, cw_v), (ein_hbm, ein_v), (eout_hbm, eout_v), (tw_hbm, tw_v),
    )
    loads = [pltpu.make_async_copy(s, d, ld_sem.at[i]) for i, (s, d) in enumerate(pairs)]
    loads[0].start()
    barrier = pltpu.get_barrier_semaphore()
    greeted = (
        [peer_a(k)[1] for k in range(1, NA)]
        + [peer_b(k)[1] for k in range(1, NB)]
        + [peer_p(k)[1] for k in range(1, NP)]
        + near
    )
    for d in greeted:
        pl.semaphore_signal(barrier, inc=1, device_id=d, device_id_type=MESH)

    sends = []

    def send(src, dst, s, r, d):
        cp = pltpu.make_async_remote_copy(src_ref=src, dst_ref=dst, send_sem=s, recv_sem=r, device_id=d, device_id_type=MESH)
        cp.start()
        sends.append(cp)
        return cp

    for cp in loads[1:5]:
        cp.start()

    def add_up(arr, b, squares):
        def body(i, carry):
            h = pl.multiple_of(i * 16, 16)
            v = in_v[arr, b, pl.ds(h, 16)].astype(f32)
            s = carry[0] + jnp.sum(v, axis=0)
            return (s, carry[1] + jnp.sum(v * v, axis=0)) if squares else (s,)

        z = jnp.zeros((W, C), f32)
        out = lax.fori_loop(0, H // 16, body, (z, z) if squares else (z,))
        return [widen(jnp.sum(o, axis=0, keepdims=True)) for o in out]

    def turn(arr):
        def body(i, _):
            h = pl.multiple_of(i * 8, 8)
            for b in range(B):
                lt[arr, b, 1:9, pl.ds(h + OWN, 8), 0:C] = jnp.transpose(in_v[arr, b, pl.ds(h, 8)].astype(f32), (1, 0, 2))
            return 0

        lax.fori_loop(0, H // 8, body, 0)

    loads[0].wait()
    for cp in loads[5:]:
        cp.start()
    sums = [add_up(0, b, True) for b in range(B)]
    a1[ia] = pack_groups(stacked([sums[0][0], sums[1][0], sums[0][1], sums[1][1]], 8))

    pl.semaphore_wait(barrier, len(greeted))

    def exchange(buf, own, sem, peers, n):
        for k in range(1, n):
            send(buf.at[own], buf.at[own], ar_s.at[sem, k], ar_r.at[sem, own], peers(k)[1])

    def gather_sum(buf, own, sem, peers, n):
        for k in range(1, n):
            j, d = peers(k)
            pltpu.make_async_remote_copy(
                src_ref=buf.at[j], dst_ref=buf.at[j], send_sem=ar_s.at[sem, k], recv_sem=ar_r.at[sem, j], device_id=d, device_id_type=MESH
            ).wait_recv()
        total = buf[0]
        for j in range(1, n):
            total = total + buf[j]
        return total

    exchange(a1, ia, 0, peer_a, NA)

    def send_halos(arr):
        halos = []

        def halo(src, dst, d):
            i = len(halos)
            halos.append(send(src, dst, halo_s.at[arr, i], halo_r.at[arr, i], d))

        halo(in_v.at[arr, :, H - 1], row_in.at[0, arr], dev_at(down, col))
        halo(in_v.at[arr, :, 0], row_in.at[1, arr], dev_at(up, col))
        turn(arr)
        for b in range(B):
            col_out[0, arr, b] = lt[arr, b, 1, OWN : OWN + H, 0:C].astype(bf16)
            col_out[1, arr, b] = lt[arr, b, W, OWN : OWN + H, 0:C].astype(bf16)
        halo(col_out.at[1, arr], col_in.at[0, arr], dev_at(row, right))
        halo(col_out.at[0, arr], col_in.at[1, arr], dev_at(row, left))
        for r in range(2):
            for c in range(2):
                i = OWN + (H - 1) * r
                for b in range(B):
                    cor_out[arr, 2 * r + c, b : b + 1, :] = lt[arr, b, 1 + (W - 1) * c, i : i + 1, :]
                halo(cor_out.at[arr, 2 * r + c], cor_in.at[arr, 2 * (1 - r) + 1 - c], dev_at((up, down)[r], (left, right)[c]))
        return halos

    def zero(i, _):
        for arr in range(2):
            for b in range(B):
                lt[arr, b, i, 0:OWN, :] = jnp.zeros((OWN, CP), f32)
                lt[arr, b, i, OWN + H :, :] = jnp.zeros((PADROWS - OWN - H, CP), f32)
                lt[arr, b, i, OWN : OWN + H, C:CP] = jnp.zeros((H, CP - C), f32)
        return 0

    lax.fori_loop(0, 10, zero, 0)
    halos_x = send_halos(0)
    loads[5].wait()
    halos_g = send_halos(1)
    gsum = [add_up(1, b, False)[0] for b in range(B)]

    loads[6].wait()
    for kw in range(3):
        for kh in range(3):
            wf[kw, kh * C : (kh + 1) * C, :] = cw_v[kh, kw]
        wf[kw, 3 * C : KP, :] = jnp.zeros((KP - 3 * C, C), bf16)

        def turn_w(i, _):
            n = pl.multiple_of(i * 64, 64)
            v = [widen(cw_v[2 - kh, 2 - kw, pl.ds(n, 64), :].astype(f32)) for kh in range(3)]

            def put(at, wide, value):
                wt[kw, pl.ds(n, 64), at : at + wide] = value.astype(bf16)

            pack_taps(put, *v)
            return 0

        lax.fori_loop(0, C // 64, turn_w, 0)
    part = max(128 // H, 1)
    for b in range(B):
        for k in range(W // part):
            v = lt[1, b, 1 + k * part : 1 + (k + 1) * part, OWN : OWN + H, :].reshape(part * H, CP)
            gt[b, :, k * part * H : (k + 1) * part * H] = jnp.transpose(v).astype(bf16)

    b1[ib] = gather_sum(a1, ia, 0, peer_a, NA)
    exchange(b1, ib, 1, peer_b, NB)

    for cp in loads[1:5] + loads[7:]:
        cp.wait()
    lane = lax.broadcasted_iota(jnp.int32, (8, C), 1)
    step = jnp.where(lane < C // 2, lane, lane - C // 2).astype(f32)
    which = lax.broadcasted_iota(jnp.int32, (8, C), 0)
    time = jnp.where(which == 0, ts_ref[0].astype(f32), ts_ref[1].astype(f32))
    angle = time * jnp.exp(-math.log(10000.0) * step / (C // 2))
    sinus = jnp.where(lane < C // 2, jnp.cos(angle), jnp.sin(angle)).astype(bf16)
    hidden = jax.nn.silu(dot(sinus, ein_v[...])).astype(bf16)
    emb = jax.nn.silu(dot(hidden, eout_v[...])).astype(bf16)
    temb = dot_nt(emb, tw_v[...]) + cb_ref[...].reshape(1, C)

    keep = [
        jnp.where(row > 0, 1.0, 0.0),
        jnp.where(row < NR - 1, 1.0, 0.0),
        jnp.where(col > 0, 1.0, 0.0),
        jnp.where(col < NC - 1, 1.0, 0.0),
    ]

    def land(arr, halos):
        for cp in halos:
            cp.wait_recv()
        for b in range(B):
            for side in range(2):
                at = OWN + H if side else TOP
                v = row_in[side, arr, b].astype(f32) * keep[side]
                for w in range(W):
                    lt[arr, b, w + 1, at : at + 1, 0:C] = v[w : w + 1]
                lt[arr, b, 9 * side, OWN : OWN + H, 0:C] = col_in[side, arr, b].astype(f32) * keep[2 + side]
                for c in range(2):
                    lt[arr, b, 9 * c, at : at + 1, :] = cor_in[arr, 2 * side + c, b : b + 1, :] * keep[side] * keep[2 + c]

    land(0, halos_x)

    def build_g(i, _):
        for b in range(B):
            for n in range(2):
                wq = i * 2 + n

                def put(at, wide, value):
                    gx[b, wq, :, at : at + wide] = value.astype(bf16)

                pack_taps(put, *(lt[1, b, wq, TOP + k : TOP + k + H, :] for k in range(3)))
        return 0

    means = spread_groups(gather_sum(b1, ib, 1, peer_b, NB)) / count
    gain, bias = widen(gain_ref[...].reshape(1, C)), widen(bias_ref[...].reshape(1, C))
    mean = [means[b : b + 1] for b in range(B)]
    rstd = [lax.rsqrt(means[B + b : B + b + 1] - mean[b] * mean[b] + EPS) for b in range(B)]
    line = lax.broadcasted_iota(jnp.int32, (PADROWS, CP), 0)
    rows_kept = jnp.where(line < OWN, keep[0], jnp.where(line < OWN + H, 1.0, keep[1]))

    def activate(b, wq, side_kept, n):
        mul = rstd[b] * gain
        normed = lt[0, b, wq] * mul + (bias - mean[b] * mul)
        sig = jax.nn.sigmoid(normed)
        t80[n] = normed * sig * (rows_kept * side_kept)

        def put(at, wide, value):
            xx[b, wq, :, at : at + wide] = value.astype(bf16)

        pack_taps(put, *(t80[n, TOP + k : TOP + k + H, :] for k in range(3)))
        return normed, sig

    def own_columns(i, _):
        for b in range(B):
            for n in range(2):
                w = i * 2 + n
                normed, sig = activate(b, w + 1, 1.0, b * 2 + n)
                normed, sig = normed[OWN : OWN + H], sig[OWN : OWN + H]
                slope[b, w] = sig * (1.0 + normed * (1.0 - sig))
        return 0

    lax.fori_loop(0, W // 2, own_columns, 0)
    for b in range(B):
        activate(b, 0, keep[2], b * 2)
        activate(b, 9, keep[3], b * 2 + 1)

    T = 3

    def third(half, kw):
        lanes = pl.ds(pl.multiple_of(half * HALF, HALF), HALF)
        r = dot(gt[0, 0:C], xx[0, kw : kw + W, :, lanes].reshape(W * H, HALF))
        return r + dot(gt[1, 0:C], xx[1, kw : kw + W, :, lanes].reshape(W * H, HALF))

    first = []
    for t in range(T):
        sb1[t] = third(1 - co, t).reshape(40, 8, HALF).astype(bf16)
        first.append(send(sb1.at[t], r1.at[t], s1_s.at[t], s1_r.at[t], dev(co_=1 - co)))
    for t in range(T):
        wg[t] = third(co, t)

    later = {}

    def to_row(t):
        first[t].wait_recv()
        for i in range(X):
            lanes = slice(i * CH, (i + 1) * CH)
            v = (wg[t, :, lanes].reshape(40, 8, CH) + r1[t, :, :, lanes].astype(f32)).reshape(Y, ZL, RB, 8, CH)
            wg2[t, i] = v
            sb2[t, i] = v.astype(bf16)
        later["x", t], later["y", t] = [], []
        for k in range(1, X):
            j = lax.rem(x + k, X)
            later["x", t].append(send(sb2.at[t, j, :, 0], rx.at[t, k], x_s.at[t, k], x_r.at[t, k], dev(x_=j)))
        for k in range(1, Y) if ZL > 1 else ():
            j = lax.rem(y + k, Y)
            later["y", t].append(send(sb2.at[t, :, j, 1], ry.at[t, k], y_s.at[t, k], y_r.at[t, k], dev(y_=j)))

    def to_other(t):
        for cp in later["x", t] + later["y", t]:
            cp.wait_recv()
        v = wg2[t, x, :, 0]
        for k in range(1, X):
            v = v + rx[t, k].astype(f32)
        wg3[t] = v
        ux[t] = v.astype(bf16)
        later["x2", t], later["y2", t] = [], []
        for k in range(1, Y):
            j = lax.rem(y + k, Y)
            later["y2", t].append(send(ux.at[t, j], vx.at[t, k], y2_s.at[t, k], y2_r.at[t, k], dev(y_=j)))
        if ZL > 1:
            v = wg2[t, :, y, 1]
            for k in range(1, Y):
                v = v + ry[t, k].astype(f32)
            wg4[t] = v
            uy[t] = v.astype(bf16)
            for k in range(1, X):
                j = lax.rem(x + k, X)
                later["x2", t].append(send(uy.at[t, j], vy.at[t, k], x2_s.at[t, k], x2_r.at[t, k], dev(x_=j)))

    for t in range(T):
        to_row(t)

    land(1, halos_g)
    lax.fori_loop(0, 5, build_g, 0)

    def dacts(i, _):
        b, w = i // 2, lax.rem(i, 2) * 4
        acc = dot_nt(gx[b, pl.ds(w, 4)].reshape(4 * H, KP), wt[0])
        for kw in range(1, 3):
            acc = acc + dot_nt(gx[b, pl.ds(w + kw, 4)].reshape(4 * H, KP), wt[kw])
        da[b, pl.ds(w, 4)] = widen(acc).reshape(4, H, CP)
        return 0

    def conv(b):
        def body(i, _):
            w = i * 4
            acc = dot(xx[b, pl.ds(w, 4)].reshape(4 * H, KP), wf[0])
            for kw in range(1, 3):
                acc = acc + dot(xx[b, pl.ds(w + kw, 4)].reshape(4 * H, KP), wf[kw])
            co_v[b, pl.ds(w, 4), :, 0:C] = acc.reshape(4, H, C)
            return 0

        lax.fori_loop(0, 2, body, 0)

        def emit(i, _):
            h = pl.multiple_of(i * 8, 8)
            v = co_v[b, :, pl.ds(h, 8), 0:C] + lt[0, b, 1:9, pl.ds(h + OWN, 8), 0:C] + temb[b : b + 1]
            ob[b, pl.ds(h, 8)] = jnp.transpose(v, (1, 0, 2)).astype(bf16)
            return 0

        lax.fori_loop(0, H // 8, emit, 0)
    lax.fori_loop(0, 3, dacts, 0)
    to_other(0)
    lax.fori_loop(3, 2 * B, dacts, 0)
    to_other(1)
    halves = []
    for b in range(B):

        def own_column(i, carry):
            s1, s2 = carry
            for n in range(2):
                w = i * 2 + n
                dn = da[b, w] * slope[b, w]
                da[b, w] = dn
                xhat = (lt[0, b, w + 1, OWN : OWN + H, :] - mean[b]) * rstd[b]
                s1 = s1 + jnp.sum(dn.reshape(H // 8, 8, CP), axis=0)
                s2 = s2 + jnp.sum((dn * xhat).reshape(H // 8, 8, CP), axis=0)
            return s1, s2

        z = jnp.zeros((8, CP), f32)
        halves.append([jnp.sum(o, axis=0, keepdims=True) for o in lax.fori_loop(0, W // 2, own_column, (z, z))])
    a2[ia] = pack_groups(stacked([halves[0][0] * gain, halves[1][0] * gain, halves[0][1] * gain, halves[1][1] * gain], 8))
    exchange(a2, ia, 2, peer_a, NA)
    a3[ia] = stacked([halves[0][0] + halves[1][0], halves[0][1] + halves[1][1], gsum[0], gsum[1]], 4)
    exchange(a3, ia, 4, peer_a, NA)
    to_other(2)
    conv(0)

    def over_z(t):
        for cp in later["x2", t] + later["y2", t]:
            cp.wait_recv()
        v = wg3[t, y]
        for k in range(1, Y):
            v = v + vx[t, k].astype(f32)
        sb3[t, 0] = v.astype(bf16)
        if ZL > 1:
            v = wg4[t, x]
            for k in range(1, X):
                v = v + vy[t, k].astype(f32)
            sb3[t, 1] = v.astype(bf16)
        for k in range(1, NZ):
            j, d = peer_z(k)
            send(sb3.at[t, lax.rem(j, ZL)], r3.at[t, iz], s3_s.at[t, k], s3_r.at[t, iz], d)
        r3[t, iz] = sb3[t, zl]

    def to_holders(t):
        for k in range(1, NZ):
            j, d = peer_z(k)
            part = r3.at[t, j]
            pltpu.make_async_remote_copy(
                src_ref=part, dst_ref=part, send_sem=s3_s.at[t, k], recv_sem=s3_r.at[t, j], device_id=d, device_id_type=MESH
            ).wait_recv()
        total = r3[t, 0].astype(f32)
        for j in range(1, NZ):
            total = total + r3[t, j].astype(f32)
        agb[t, ip] = total.astype(bf16)
        for k in range(1, NP):
            send(agb.at[t, ip], agb.at[t, ip], ag_s.at[t, k], ag_r.at[t, ip], peer_p(k)[1])

    over_z(0)
    over_z(1)
    b2[ib] = gather_sum(a2, ia, 2, peer_a, NA)
    exchange(b2, ib, 3, peer_b, NB)
    b3[ib] = gather_sum(a3, ia, 4, peer_a, NA)
    exchange(b3, ib, 5, peer_b, NB)
    over_z(2)
    conv(1)
    to_holders(0)
    to_holders(1)
    to_holders(2)

    groups = spread_groups(gather_sum(b2, ib, 3, peer_b, NB)) / count
    totals = gather_sum(b3, ib, 5, peer_b, NB)
    for b in range(B):
        m1, m2 = groups[b : b + 1, 0:C], groups[B + b : B + b + 1, 0:C]
        mb, rb = mean[b][:, 0:C], rstd[b][:, 0:C]

        def emit(i, _):
            h = pl.multiple_of(i * 8, 8)
            xv = lt[0, b, 1:9, pl.ds(h + OWN, 8), 0:C]
            gv = lt[1, b, 1:9, pl.ds(h + OWN, 8), 0:C]
            dn = da[b, :, pl.ds(h, 8), 0:C]
            v = gv + rb * (dn * gain[:, 0:C] - m1 - (xv - mb) * rb * m2)
            og[b, pl.ds(h, 8)] = jnp.transpose(v, (1, 0, 2))
            return 0

        lax.fori_loop(0, H // 8, emit, 0)
    st_ref[...] = (stacked([totals[1:2], totals[0:1], totals[2:3] + totals[3:4]], 8) * scale)[:, 0:C]
    g2 = jnp.concatenate([totals[2:3], totals[3:4]], axis=0)[:, 0:C]
    hi = g2.astype(bf16)
    rest = g2 - hi.astype(f32)
    mid = rest.astype(bf16)
    low = (rest - mid.astype(f32)).astype(bf16)
    e2 = emb[0:B].astype(f32)
    left_rows = jnp.concatenate([hi.astype(f32), mid.astype(f32), low.astype(f32), jnp.zeros((2, C), f32)], axis=0)
    right_rows = jnp.concatenate([e2, e2, e2, jnp.zeros((2, TE), f32)], axis=0).astype(bf16)
    twg_ref[...] = dot(jnp.transpose(left_rows).astype(bf16), right_rows) * scale

    for t in range(T):
        for k in range(1, NP):
            j, d = peer_p(k)
            part = agb.at[t, j]
            pltpu.make_async_remote_copy(
                src_ref=part, dst_ref=part, send_sem=ag_s.at[t, k], recv_sem=ag_r.at[t, j], device_id=d, device_id_type=MESH
            ).wait_recv()
        full = jnp.concatenate([agb[t, p].astype(f32).reshape(RB * 8, CH) for p in range(NP)], axis=1) * scale
        cwg_ref[0, t] = full[:, 0:C]
        cwg_ref[1, t] = pltpu.roll(full[:, 256:640], CP - 64, 1)[:, 0:C]
        cwg_ref[2, t] = full[:, 2 * C : 3 * C]
    for cp in sends:
        cp.wait_send()


def write_out(ob, og, cwg, st, twg, bo_hbm, ig_hbm, cwg_hbm, twg_hbm, gg_ref, bg_ref, cbg_ref, sem):
    pairs = ((twg, twg_hbm), (og, ig_hbm), (ob, bo_hbm), (cwg, cwg_hbm))
    copies = [pltpu.make_async_copy(s, d, sem.at[i]) for i, (s, d) in enumerate(pairs)]
    for cp in copies:
        cp.start()
    for i, ref in enumerate((gg_ref, bg_ref, cbg_ref)):
        ref[...] = st[i : i + 1, :].reshape(C)
    for cp in copies:
        cp.wait()


def step(sizes, latent, timestep, gain, bias, conv_w, conv_b, embed_in, embed_out, time_w, cotangent):
    Y, ZL, X, ZH, CO = sizes
    H = latent.shape[1]
    NA, NB, NP, NZ = ZH * ZL * CO, X * Y, CO * X, ZH * ZL
    HALF = KP // CO
    CH = HALF // X
    RB = 40 // (Y * ZL)
    T = 3
    anyspace = pl.BlockSpec(memory_space=pl.ANY)
    vmem = pl.BlockSpec(memory_space=pltpu.VMEM)
    V, D = pltpu.VMEM, pltpu.SemaphoreType.DMA
    NG = max(NA, NB)
    held = pl.pallas_call(
        functools.partial(kernel, sizes, H),
        out_shape=(
            HELD((B, H, W, C), bf16),
            HELD((B, H, W, C), f32),
            HELD((3, 3, RB * 8, C), f32),
            HELD((8, C), f32),
            HELD((C, TE), f32),
        ),
        in_specs=[anyspace] * 10,
        out_specs=(vmem,) * 5,
        scratch_shapes=[
            pltpu.SMEM((B,), jnp.int32),
            V((C,), f32),
            V((C,), f32),
            V((C,), f32),
            V((2, B, H, W, C), bf16),
            V((3, 3, C, C), bf16),
            V((C, TE), bf16),
            V((TE, TE), bf16),
            V((C, TE), bf16),
            V((2, 2, B, W, C), bf16),
            V((2, 2, B, H, C), bf16),
            V((2, 2, B, H, C), bf16),
            V((2, 4, 8, CP), f32),
            V((2, 4, 8, CP), f32),
            V((2, B, 10, PADROWS, CP), f32),
            V((4, PADROWS, CP), f32),
            V((B, 10, H, KP), bf16),
            V((B, 10, H, KP), bf16),
            V((3, KP, C), bf16),
            V((3, C, KP), bf16),
            V((B, W, H, CP), f32),
            V((B, W, H, CP), f32),
            V((B, CP, W * H), bf16),
            V((T, C, HALF), f32),
            V((T, X, Y, ZL, RB, 8, CH), f32),
            V((T, Y, RB, 8, CH), f32),
            V((T, X, RB, 8, CH), f32),
            V((T, 40, 8, HALF), bf16),
            V((T, 40, 8, HALF), bf16),
            V((T, X, Y, ZL, RB, 8, CH), bf16),
            V((T, X, Y, RB, 8, CH), bf16),
            V((T, Y, X, RB, 8, CH), bf16),
            V((T, Y, RB, 8, CH), bf16),
            V((T, X, RB, 8, CH), bf16),
            V((T, Y, RB, 8, CH), bf16),
            V((T, X, RB, 8, CH), bf16),
            V((T, ZL, RB, 8, CH), bf16),
            V((T, NZ, RB, 8, CH), bf16),
            V((T, NP, RB, 8, CH), bf16),
            V((B, W, H, CP), f32),
            V((NA, 1, 128), f32),
            V((NB, 1, 128), f32),
            V((NA, 1, 128), f32),
            V((NB, 1, 128), f32),
            V((NA, 4, CP), f32),
            V((NB, 4, CP), f32),
            D((10,)),
            D((2, 8)),
            D((2, 8)),
            D((6, NG)),
            D((6, NG)),
            D((T,)),
            D((T,)),
            D((T, X)),
            D((T, X)),
            D((T, Y)),
            D((T, Y)),
            D((T, X)),
            D((T, X)),
            D((T, Y)),
            D((T, Y)),
            D((T, NZ)),
            D((T, NZ)),
            D((T, NP)),
            D((T, NP)),
        ],
        compiler_params=pltpu.CompilerParams(collective_id=0, has_side_effects=True, vmem_limit_bytes=LIMIT),
        name="block",
    )(timestep, gain, bias, conv_b, latent, cotangent, conv_w, embed_in, embed_out, time_w.T)
    bo, ig, cwg, twg, gg, bg, cbg = pl.pallas_call(
        write_out,
        out_shape=(
            jax.ShapeDtypeStruct((B, H, W, C), bf16),
            jax.ShapeDtypeStruct((B, H, W, C), f32),
            jax.ShapeDtypeStruct((3, 3, RB * 8, C), f32),
            jax.ShapeDtypeStruct((C, TE), f32),
            jax.ShapeDtypeStruct((C,), f32),
            jax.ShapeDtypeStruct((C,), f32),
            jax.ShapeDtypeStruct((C,), f32),
        ),
        in_specs=[vmem] * 5,
        out_specs=(anyspace,) * 4 + (vmem,) * 3,
        scratch_shapes=[D((4,))],
        compiler_params=pltpu.CompilerParams(vmem_limit_bytes=1024 * 1024),
        name="write_out",
    )(*held)
    return bo, ig, cwg.transpose(2, 0, 1, 3), gg, bg, cbg, twg.T


def build(finer):
    sizes = tuple(finer.shape[a] for a in AXES)
    image = P(None, ROW, COL, None)
    return jax.shard_map(
        functools.partial(step, sizes),
        mesh=finer,
        in_specs=(image, P(), P(), P(), P(), P(), P(), P(), P(), image),
        out_specs=(image, image, P(ROW, None, None, None), P(), P(), P(), P()),
        check_vma=False,
    )


def solution(mesh):
    return build(Mesh(mesh.devices.reshape(4, 2, 4, 4, 2), AXES))
```

```python
import functools
import math

import jax
import jax.numpy as jnp
from jax import lax
from jax.experimental import pallas as pl
from jax.experimental.pallas import tpu as pltpu
from jax.sharding import Mesh
from jax.sharding import PartitionSpec as P

AXES = ("row_0", "row_1", "col_0", "col_1", "col_2")
ROW = ("row_0", "row_1")
COL = ("col_0", "col_1", "col_2")
EPS = 1e-05
GROUP = 10
C, CP = 320, 384
TE = 1280
B = 2
W = 8
TOP, OWN, PADROWS = 7, 8, 80
KP = 1024
f32, bf16 = jnp.float32, jnp.bfloat16
MESH = pl.DeviceIdType.MESH
HELD = pltpu.VMEM
LIMIT = 50 * 1024 * 1024


def widen(v):
    return jnp.concatenate([v, jnp.zeros(v.shape[:-1] + (CP - C,), v.dtype)], axis=-1)


def dot(a, b):
    return jnp.dot(a, b, preferred_element_type=f32)


def dot_nt(a, b):
    return lax.dot_general(a, b, (((1,), (1,)), ((), ())), preferred_element_type=f32)


def pack_taps(put, v0, v1, v2):
    r = pltpu.roll(v1, 64, 1)
    put(0, 256, v0[:, 0:256])
    put(256, 128, v0[:, 256:384] + r[:, 0:128])
    put(384, 256, r[:, 128:384])
    put(640, 384, v2)


def dot_exact(v, ones):
    hi = v.astype(bf16)
    rest = v - hi.astype(f32)
    mid = rest.astype(bf16)
    low = (rest - mid.astype(f32)).astype(bf16)
    return dot(hi, ones) + dot(mid, ones) + dot(low, ones)


def own_lanes():
    r = lax.broadcasted_iota(jnp.int32, (8, 128), 0)
    lane = lax.broadcasted_iota(jnp.int32, (8, 128), 1)
    return (lane >> 5) == r


def pack_groups(v):
    c = lax.broadcasted_iota(jnp.int32, (CP, 128), 0)
    lane = lax.broadcasted_iota(jnp.int32, (CP, 128), 1)
    ones = jnp.where((((c * 6554) >> 16) == (lane & 31)) & (c < C), 1.0, 0.0).astype(bf16)
    return jnp.sum(jnp.where(own_lanes(), dot_exact(v, ones), 0.0), axis=0, keepdims=True)


def spread_groups(t):
    lane = lax.broadcasted_iota(jnp.int32, (128, CP), 0)
    c = lax.broadcasted_iota(jnp.int32, (128, CP), 1)
    ones = jnp.where((((c * 6554) >> 16) == (lane & 31)) & (c < C), 1.0, 0.0).astype(bf16)
    return dot_exact(jnp.where(own_lanes(), jnp.broadcast_to(t, (8, 128)), 0.0), ones)


def stacked(rows, n):
    return jnp.concatenate(rows + [jnp.zeros((n - len(rows), CP), f32)], axis=0) if len(rows) < n else jnp.concatenate(rows, axis=0)


def kernel(
    sizes,
    H,
    ts_hbm, gain_hbm, bias_hbm, cb_hbm, lat_hbm, cot_hbm, cw_hbm, ein_hbm, eout_hbm, tw_hbm,
    ob, og, cwg_ref, st_ref, twg_ref,
    ts_ref, gain_ref, bias_ref, cb_ref,
    in_v, cw_v, ein_v, eout_v, tw_v,
    row_in, col_out, col_in, cor_out, cor_in,
    lt, t80, gx, xx, wf, wt, da, co_v, gt, wg, wg2, wg3, wg4,
    sb1, r1, sb2, rx, ry, ux, uy, vx, vy, sb3, r3, agb, slope,
    a1, b1, a2, b2, a3, b3, a4, b4,
    ld_sem, halo_s, halo_r, ar_s, ar_r, s1_s, s1_r, x_s, x_r, y_s, y_r, x2_s, x2_r, y2_s, y2_r, s3_s, s3_r, ag_s, ag_r,
):
    Y, ZL, X, ZH, CO = sizes
    y, zl, x, zh, co = (lax.axis_index(a) for a in AXES)
    row, col = y * ZL + zl, (x * ZH + zh) * CO + co
    NR, NC = Y * ZL, X * ZH * CO
    NA, NB, NP, NZ = ZH * ZL * CO, X * Y, CO * X, ZH * ZL
    HALF = KP // CO
    CH = HALF // X
    RB = 40 // NR
    count = float(GROUP * H * NR * W * NC)
    scale = 1.0 / math.sqrt(B * H * NR * W * NC)

    def dev(y_=None, zl_=None, x_=None, zh_=None, co_=None):
        return {
            "row_0": y if y_ is None else y_,
            "row_1": zl if zl_ is None else zl_,
            "col_0": x if x_ is None else x_,
            "col_1": zh if zh_ is None else zh_,
            "col_2": co if co_ is None else co_,
        }

    def dev_at(r, c):
        return dev(r // ZL, lax.rem(r, ZL), c // (ZH * CO), lax.rem(c // CO, ZH), lax.rem(c, CO))

    ia, ib, iz, ip = (zh * ZL + zl) * CO + co, x * Y + y, zh * ZL + zl, co * X + x

    def peer_a(k):
        j = lax.rem(ia + k, NA)
        return j, dev(zl_=lax.rem(j // CO, ZL), zh_=j // (CO * ZL), co_=lax.rem(j, CO))

    def peer_b(k):
        j = lax.rem(ib + k, NB)
        return j, dev(x_=j // Y, y_=lax.rem(j, Y))

    def peer_z(k):
        j = lax.rem(iz + k, NZ)
        return j, dev(zl_=lax.rem(j, ZL), zh_=j // ZL)

    def peer_p(k):
        j = lax.rem(ip + k, NP)
        return j, dev(co_=j // X, x_=lax.rem(j, X))

    up, down = lax.rem(row + NR - 1, NR), lax.rem(row + 1, NR)
    left, right = lax.rem(col + NC - 1, NC), lax.rem(col + 1, NC)
    near = [dev_at(r, c) for r in (up, row, down) for c in (left, col, right) if not (r is row and c is col)]

    pairs = (
        (lat_hbm.at[0], in_v.at[0, 0]), (ts_hbm, ts_ref), (gain_hbm, gain_ref), (bias_hbm, bias_ref), (cb_hbm, cb_ref),
        (cot_hbm, in_v.at[1]), (cw_hbm, cw_v), (ein_hbm, ein_v), (eout_hbm, eout_v), (tw_hbm, tw_v),
        (lat_hbm.at[1], in_v.at[0, 1]),
    )
    loads = [pltpu.make_async_copy(s, d, ld_sem.at[i]) for i, (s, d) in enumerate(pairs)]
    loads[0].start()
    loads[10].start()
    barrier = pltpu.get_barrier_semaphore()
    greeted = (
        [peer_a(k)[1] for k in range(1, NA)]
        + [peer_b(k)[1] for k in range(1, NB)]
        + [dev(x_=lax.rem(x + k, X), co_=1 - co) for k in range(1, X)]
        + near
    )
    for d in greeted:
        pl.semaphore_signal(barrier, inc=1, device_id=d, device_id_type=MESH)

    sends = []

    def send(src, dst, s, r, d):
        cp = pltpu.make_async_remote_copy(src_ref=src, dst_ref=dst, send_sem=s, recv_sem=r, device_id=d, device_id_type=MESH)
        cp.start()
        sends.append(cp)
        return cp

    for cp in loads[1:5]:
        cp.start()

    def add_up(arr, b, squares):
        def body(i, carry):
            h = pl.multiple_of(i * 16, 16)
            v = in_v[arr, b, pl.ds(h, 16)].astype(f32)
            s = carry[0] + jnp.sum(v, axis=0)
            return (s, carry[1] + jnp.sum(v * v, axis=0)) if squares else (s,)

        z = jnp.zeros((W, C), f32)
        out = lax.fori_loop(0, H // 16, body, (z, z) if squares else (z,))
        return [widen(jnp.sum(o, axis=0, keepdims=True)) for o in out]

    def turn(arr):
        def body(i, _):
            h = pl.multiple_of(i * 8, 8)
            for b in range(B):
                lt[arr, b, 1:9, pl.ds(h + OWN, 8), 0:C] = jnp.transpose(in_v[arr, b, pl.ds(h, 8)].astype(f32), (1, 0, 2))
            return 0

        lax.fori_loop(0, H // 8, body, 0)

    loads[0].wait()
    sums = [add_up(0, 0, True)]
    loads[10].wait()
    for cp in loads[5:10]:
        cp.start()
    sums.append(add_up(0, 1, True))
    a1[ia] = pack_groups(stacked([sums[0][0], sums[1][0], sums[0][1], sums[1][1]], 8))

    pl.semaphore_wait(barrier, len(greeted))

    def fan(copies, s, r, whole):
        for src, dst, d in copies:
            pltpu.make_async_remote_copy(src_ref=src, dst_ref=dst, send_sem=s, recv_sem=r, device_id=d, device_id_type=MESH).start()
        every = pltpu.make_async_remote_copy(
            src_ref=whole, dst_ref=whole, send_sem=s, recv_sem=r, device_id=copies[0][2], device_id_type=MESH
        )
        sends.append(every)
        return every

    arrivals = {}

    def exchange(buf, own, sem, peers, n):
        part = buf.at[own]
        arrivals[sem] = fan(
            [(part, part, peers(k)[1]) for k in range(1, n)], ar_s.at[sem], ar_r.at[sem], buf.at[pl.ds(0, n - 1)]
        )

    def gather_sum(buf, sem, n):
        arrivals[sem].wait_recv()
        total = buf[0]
        for j in range(1, n):
            total = total + buf[j]
        return total

    exchange(a1, ia, 0, peer_a, NA)

    def send_halos(arr):
        halos = []

        def halo(src, dst, d):
            i = len(halos)
            halos.append(send(src, dst, halo_s.at[arr, i], halo_r.at[arr, i], d))

        halo(in_v.at[arr, :, H - 1], row_in.at[0, arr], dev_at(down, col))
        halo(in_v.at[arr, :, 0], row_in.at[1, arr], dev_at(up, col))
        turn(arr)
        for b in range(B):
            col_out[0, arr, b] = lt[arr, b, 1, OWN : OWN + H, 0:C].astype(bf16)
            col_out[1, arr, b] = lt[arr, b, W, OWN : OWN + H, 0:C].astype(bf16)
        halo(col_out.at[1, arr], col_in.at[0, arr], dev_at(row, right))
        halo(col_out.at[0, arr], col_in.at[1, arr], dev_at(row, left))
        for r in range(2):
            for c in range(2):
                i = OWN + (H - 1) * r
                for b in range(B):
                    cor_out[arr, 2 * r + c, b : b + 1, :] = lt[arr, b, 1 + (W - 1) * c, i : i + 1, :]
                halo(cor_out.at[arr, 2 * r + c], cor_in.at[arr, 2 * (1 - r) + 1 - c], dev_at((up, down)[r], (left, right)[c]))
        return halos

    def zero(i, _):
        for arr in range(2):
            for b in range(B):
                lt[arr, b, i, 0:OWN, :] = jnp.zeros((OWN, CP), f32)
                lt[arr, b, i, OWN + H :, :] = jnp.zeros((PADROWS - OWN - H, CP), f32)
                lt[arr, b, i, OWN : OWN + H, C:CP] = jnp.zeros((H, CP - C), f32)
        return 0

    lax.fori_loop(0, 10, zero, 0)
    halos_x = send_halos(0)
    loads[5].wait()
    halos_g = send_halos(1)
    gsum = [add_up(1, b, False)[0] for b in range(B)]

    loads[6].wait()
    for kw in range(3):
        for kh in range(3):
            wf[kw, kh * C : (kh + 1) * C, :] = cw_v[kh, kw]
        wf[kw, 3 * C : KP, :] = jnp.zeros((KP - 3 * C, C), bf16)

        def turn_w(i, _):
            n = pl.multiple_of(i * 64, 64)
            v = [widen(cw_v[2 - kh, 2 - kw, pl.ds(n, 64), :].astype(f32)) for kh in range(3)]

            def put(at, wide, value):
                wt[kw, pl.ds(n, 64), at : at + wide] = value.astype(bf16)

            pack_taps(put, *v)
            return 0

        lax.fori_loop(0, C // 64, turn_w, 0)
    part = max(128 // H, 1)
    for b in range(B):
        for k in range(W // part):
            v = lt[1, b, 1 + k * part : 1 + (k + 1) * part, OWN : OWN + H, :].reshape(part * H, CP)
            gt[b, :, k * part * H : (k + 1) * part * H] = jnp.transpose(v).astype(bf16)

    b1[ib] = gather_sum(a1, 0, NA)
    exchange(b1, ib, 1, peer_b, NB)
    a4[ia] = jnp.concatenate(gsum, axis=0)
    exchange(a4, ia, 6, peer_a, NA)

    for cp in loads[1:5] + loads[7:10]:
        cp.wait()
    lane = lax.broadcasted_iota(jnp.int32, (8, C), 1)
    step = jnp.where(lane < C // 2, lane, lane - C // 2).astype(f32)
    which = lax.broadcasted_iota(jnp.int32, (8, C), 0)
    time = jnp.where(which == 0, ts_ref[0].astype(f32), ts_ref[1].astype(f32))
    angle = time * jnp.exp(-math.log(10000.0) * step / (C // 2))
    sinus = jnp.where(lane < C // 2, jnp.cos(angle), jnp.sin(angle)).astype(bf16)
    hidden = jax.nn.silu(dot(sinus, ein_v[...])).astype(bf16)
    emb = jax.nn.silu(dot(hidden, eout_v[...])).astype(bf16)
    temb = dot_nt(emb, tw_v[...]) + cb_ref[...].reshape(1, C)

    keep = [
        jnp.where(row > 0, 1.0, 0.0),
        jnp.where(row < NR - 1, 1.0, 0.0),
        jnp.where(col > 0, 1.0, 0.0),
        jnp.where(col < NC - 1, 1.0, 0.0),
    ]

    def land(arr, halos):
        for cp in halos:
            cp.wait_recv()
        for b in range(B):
            for side in range(2):
                at = OWN + H if side else TOP
                v = row_in[side, arr, b].astype(f32) * keep[side]
                for w in range(W):
                    lt[arr, b, w + 1, at : at + 1, 0:C] = v[w : w + 1]
                lt[arr, b, 9 * side, OWN : OWN + H, 0:C] = col_in[side, arr, b].astype(f32) * keep[2 + side]
                for c in range(2):
                    lt[arr, b, 9 * c, at : at + 1, :] = cor_in[arr, 2 * side + c, b : b + 1, :] * keep[side] * keep[2 + c]

    land(0, halos_x)

    def build_g(i, _):
        for b in range(B):
            for n in range(2):
                wq = i * 2 + n

                def put(at, wide, value):
                    gx[b, wq, :, at : at + wide] = value.astype(bf16)

                pack_taps(put, *(lt[1, b, wq, TOP + k : TOP + k + H, :] for k in range(3)))
        return 0

    means = spread_groups(gather_sum(b1, 1, NB)) / count
    gain, bias = widen(gain_ref[...].reshape(1, C)), widen(bias_ref[...].reshape(1, C))
    mean = [means[b : b + 1] for b in range(B)]
    rstd = [lax.rsqrt(means[B + b : B + b + 1] - mean[b] * mean[b] + EPS) for b in range(B)]
    line = lax.broadcasted_iota(jnp.int32, (PADROWS, CP), 0)
    rows_kept = jnp.where(line < OWN, keep[0], jnp.where(line < OWN + H, 1.0, keep[1]))

    def activate(b, wq, side_kept, n):
        mul = rstd[b] * gain
        normed = lt[0, b, wq] * mul + (bias - mean[b] * mul)
        sig = jax.nn.sigmoid(normed)
        t80[n] = normed * sig * (rows_kept * side_kept)

        def put(at, wide, value):
            xx[b, wq, :, at : at + wide] = value.astype(bf16)

        pack_taps(put, *(t80[n, TOP + k : TOP + k + H, :] for k in range(3)))
        return normed, sig

    def own_columns(i, _):
        for b in range(B):
            for n in range(2):
                w = i * 2 + n
                normed, sig = activate(b, w + 1, 1.0, b * 2 + n)
                normed, sig = normed[OWN : OWN + H], sig[OWN : OWN + H]
                slope[b, w] = sig * (1.0 + normed * (1.0 - sig))
        return 0

    lax.fori_loop(0, W // 2, own_columns, 0)
    for b in range(B):
        activate(b, 0, keep[2], b * 2)
        activate(b, 9, keep[3], b * 2 + 1)

    T = 3

    def third(half, kw):
        lanes = pl.ds(pl.multiple_of(half * HALF, HALF), HALF)
        r = dot(gt[0, 0:C], xx[0, kw : kw + W, :, lanes].reshape(W * H, HALF))
        return r + dot(gt[1, 0:C], xx[1, kw : kw + W, :, lanes].reshape(W * H, HALF))

    first = []
    for t in range(T):
        sb1[t] = third(1 - co, t).reshape(40, 8, HALF).astype(bf16)
        first.append(send(sb1.at[t], r1.at[t], s1_s.at[t], s1_r.at[t], dev(co_=1 - co)))

    later = {}

    def to_row(t):
        first[t].wait_recv()
        for i in range(X):
            lanes = slice(i * CH, (i + 1) * CH)
            v = (wg[t, :, lanes].reshape(40, 8, CH) + r1[t, :, :, lanes].astype(f32)).reshape(Y, ZL, RB, 8, CH)
            wg2[t, i] = v
            sb2[t, i] = v.astype(bf16)
        peers = [lax.rem(x + k, X) for k in range(1, X)]
        later["x", t] = fan(
            [(sb2.at[t, j, :, 0], rx.at[t, k], dev(x_=j)) for k, j in enumerate(peers)],
            x_s.at[t], x_r.at[t], rx.at[t],
        )
        if ZL > 1:
            peers = [lax.rem(y + k, Y) for k in range(1, Y)]
            later["y", t] = fan(
                [(sb2.at[t, :, j, 1], ry.at[t, k], dev(y_=j)) for k, j in enumerate(peers)],
                y_s.at[t], y_r.at[t], ry.at[t],
            )

    def to_other(t):
        later["x", t].wait_recv()
        v = wg2[t, x, :, 0]
        for k in range(X - 1):
            v = v + rx[t, k].astype(f32)
        wg3[t] = v
        ux[t] = v.astype(bf16)
        peers = [lax.rem(y + k, Y) for k in range(1, Y)]
        later["y2", t] = fan(
            [(ux.at[t, j], vx.at[t, k], dev(y_=j)) for k, j in enumerate(peers)], y2_s.at[t], y2_r.at[t], vx.at[t]
        )
        if ZL > 1:
            later["y", t].wait_recv()
            v = wg2[t, :, y, 1]
            for k in range(Y - 1):
                v = v + ry[t, k].astype(f32)
            wg4[t] = v
            uy[t] = v.astype(bf16)
            peers = [lax.rem(x + k, X) for k in range(1, X)]
            later["x2", t] = fan(
                [(uy.at[t, j], vy.at[t, k], dev(x_=j)) for k, j in enumerate(peers)], x2_s.at[t], x2_r.at[t], vy.at[t]
            )

    for t in range(T):
        wg[t] = third(co, t)
        to_row(t)

    b4[ib] = gather_sum(a4, 6, NA)
    exchange(b4, ib, 7, peer_b, NB)
    land(1, halos_g)
    lax.fori_loop(0, 5, build_g, 0)

    def dacts(i, _):
        b, w = i // 2, lax.rem(i, 2) * 4
        acc = dot_nt(gx[b, pl.ds(w, 4)].reshape(4 * H, KP), wt[0])
        for kw in range(1, 3):
            acc = acc + dot_nt(gx[b, pl.ds(w + kw, 4)].reshape(4 * H, KP), wt[kw])
        da[b, pl.ds(w, 4)] = widen(acc).reshape(4, H, CP)
        return 0

    def conv(b, half):
        w = half * 4
        acc = dot(xx[b, w : w + 4].reshape(4 * H, KP), wf[0])
        for kw in range(1, 3):
            acc = acc + dot(xx[b, w + kw : w + kw + 4].reshape(4 * H, KP), wf[kw])
        co_v[b, w : w + 4, :, 0:C] = acc.reshape(4, H, C)

    def emit_block(b):
        def emit(i, _):
            h = pl.multiple_of(i * 8, 8)
            v = co_v[b, :, pl.ds(h, 8), 0:C] + lt[0, b, 1:9, pl.ds(h + OWN, 8), 0:C] + temb[b : b + 1]
            ob[b, pl.ds(h, 8)] = jnp.transpose(v, (1, 0, 2)).astype(bf16)
            return 0

        lax.fori_loop(0, H // 8, emit, 0)

    lax.fori_loop(0, 2, dacts, 0)
    to_other(0)
    lax.fori_loop(2, 3, dacts, 0)
    to_other(1)
    lax.fori_loop(3, 2 * B, dacts, 0)
    halves = []
    for b in range(B):

        def own_column(i, carry):
            s1, s2 = carry
            for n in range(2):
                w = i * 2 + n
                dn = da[b, w] * slope[b, w]
                da[b, w] = dn
                xhat = (lt[0, b, w + 1, OWN : OWN + H, :] - mean[b]) * rstd[b]
                s1 = s1 + jnp.sum(dn.reshape(H // 8, 8, CP), axis=0)
                s2 = s2 + jnp.sum((dn * xhat).reshape(H // 8, 8, CP), axis=0)
            return s1, s2

        z = jnp.zeros((8, CP), f32)
        halves.append([jnp.sum(o, axis=0, keepdims=True) for o in lax.fori_loop(0, W // 2, own_column, (z, z))])
    a2[ia] = pack_groups(stacked([halves[0][0] * gain, halves[1][0] * gain, halves[0][1] * gain, halves[1][1] * gain], 8))
    exchange(a2, ia, 2, peer_a, NA)
    a3[ia] = jnp.concatenate([halves[0][0] + halves[1][0], halves[0][1] + halves[1][1]], axis=0)
    exchange(a3, ia, 4, peer_a, NA)
    to_other(2)
    def time_grad():
        hi = gtotal[:, 0:C].astype(bf16)
        rest = gtotal[:, 0:C] - hi.astype(f32)
        mid = rest.astype(bf16)
        low = (rest - mid.astype(f32)).astype(bf16)
        e2 = emb[0:B].astype(f32)
        left_rows = jnp.concatenate([hi.astype(f32), mid.astype(f32), low.astype(f32), jnp.zeros((2, C), f32)], axis=0)
        right_rows = jnp.concatenate([e2, e2, e2, jnp.zeros((2, TE), f32)], axis=0).astype(bf16)
        return dot(jnp.transpose(left_rows).astype(bf16), right_rows) * scale

    def over_z(t):
        later["y2", t].wait_recv()
        v = wg3[t, y]
        for k in range(Y - 1):
            v = v + vx[t, k].astype(f32)
        sb3[t, 0] = v.astype(bf16)
        if ZL > 1:
            later["x2", t].wait_recv()
            v = wg4[t, x]
            for k in range(X - 1):
                v = v + vy[t, k].astype(f32)
            sb3[t, 1] = v.astype(bf16)
        peers = [peer_z(k) for k in range(1, NZ)]
        later["z", t] = fan(
            [(sb3.at[t, lax.rem(j, ZL)], r3.at[t, iz], d) for j, d in peers], s3_s.at[t], s3_r.at[t], r3.at[t, pl.ds(0, NZ - 1)]
        )
        r3[t, iz] = sb3[t, zl]

    def to_holders(t):
        later["z", t].wait_recv()
        total = r3[t, 0].astype(f32)
        for j in range(1, NZ):
            total = total + r3[t, j].astype(f32)
        agb[t, ip] = total.astype(bf16)
        part = agb.at[t, ip]
        later["p", t] = fan(
            [(part, part, peer_p(k)[1]) for k in range(1, NP)], ag_s.at[t], ag_r.at[t], agb.at[t, pl.ds(0, NP - 1)]
        )

    over_z(0)
    conv(0, 0)
    over_z(1)
    conv(0, 1)
    emit_block(0)
    over_z(2)
    conv(1, 0)
    conv(1, 1)
    emit_block(1)
    b2[ib] = gather_sum(a2, 2, NA)
    exchange(b2, ib, 3, peer_b, NB)
    b3[ib] = gather_sum(a3, 4, NA)
    exchange(b3, ib, 5, peer_b, NB)
    to_holders(0)
    gtotal = gather_sum(b4, 7, NB)
    twg_ref[...] = time_grad()
    to_holders(1)
    to_holders(2)

    groups = spread_groups(gather_sum(b2, 3, NB)) / count
    totals = gather_sum(b3, 5, NB)
    for b in range(B):
        m1, m2 = groups[b : b + 1, 0:C], groups[B + b : B + b + 1, 0:C]
        mb, rb = mean[b][:, 0:C], rstd[b][:, 0:C]

        def emit(i, _):
            h = pl.multiple_of(i * 8, 8)
            xv = lt[0, b, 1:9, pl.ds(h + OWN, 8), 0:C]
            gv = lt[1, b, 1:9, pl.ds(h + OWN, 8), 0:C]
            dn = da[b, :, pl.ds(h, 8), 0:C]
            v = gv + rb * (dn * gain[:, 0:C] - m1 - (xv - mb) * rb * m2)
            og[b, pl.ds(h, 8)] = jnp.transpose(v, (1, 0, 2))
            return 0

        lax.fori_loop(0, H // 8, emit, 0)
    st_ref[...] = (stacked([totals[1:2], totals[0:1], gtotal[0:1] + gtotal[1:2]], 8) * scale)[:, 0:C]
    for t in range(T):
        later["p", t].wait_recv()
        full = jnp.concatenate([agb[t, p].astype(f32).reshape(RB * 8, CH) for p in range(NP)], axis=1) * scale
        cwg_ref[0, t] = full[:, 0:C]
        cwg_ref[1, t] = pltpu.roll(full[:, 256:640], CP - 64, 1)[:, 0:C]
        cwg_ref[2, t] = full[:, 2 * C : 3 * C]
    for cp in sends:
        cp.wait_send()


def write_out(ob, og, cwg, st, twg, bo_hbm, ig_hbm, cwg_hbm, twg_hbm, gg_ref, bg_ref, cbg_ref, sem):
    pairs = ((twg, twg_hbm), (og, ig_hbm), (ob, bo_hbm), (cwg, cwg_hbm))
    copies = [pltpu.make_async_copy(s, d, sem.at[i]) for i, (s, d) in enumerate(pairs)]
    for cp in copies:
        cp.start()
    for i, ref in enumerate((gg_ref, bg_ref, cbg_ref)):
        ref[...] = st[i : i + 1, :].reshape(C)
    for cp in copies:
        cp.wait()


def step(sizes, latent, timestep, gain, bias, conv_w, conv_b, embed_in, embed_out, time_w, cotangent):
    Y, ZL, X, ZH, CO = sizes
    H = latent.shape[1]
    NA, NB, NP, NZ = ZH * ZL * CO, X * Y, CO * X, ZH * ZL
    HALF = KP // CO
    CH = HALF // X
    RB = 40 // (Y * ZL)
    T = 3
    anyspace = pl.BlockSpec(memory_space=pl.ANY)
    vmem = pl.BlockSpec(memory_space=pltpu.VMEM)
    V, D = pltpu.VMEM, pltpu.SemaphoreType.DMA
    held = pl.pallas_call(
        functools.partial(kernel, sizes, H),
        out_shape=(
            HELD((B, H, W, C), bf16),
            HELD((B, H, W, C), f32),
            HELD((3, 3, RB * 8, C), f32),
            HELD((8, C), f32),
            HELD((C, TE), f32),
        ),
        in_specs=[anyspace] * 10,
        out_specs=(vmem,) * 5,
        scratch_shapes=[
            pltpu.SMEM((B,), jnp.int32),
            V((C,), f32),
            V((C,), f32),
            V((C,), f32),
            V((2, B, H, W, C), bf16),
            V((3, 3, C, C), bf16),
            V((C, TE), bf16),
            V((TE, TE), bf16),
            V((C, TE), bf16),
            V((2, 2, B, W, C), bf16),
            V((2, 2, B, H, C), bf16),
            V((2, 2, B, H, C), bf16),
            V((2, 4, 8, CP), f32),
            V((2, 4, 8, CP), f32),
            V((2, B, 10, PADROWS, CP), f32),
            V((4, PADROWS, CP), f32),
            V((B, 10, H, KP), bf16),
            V((B, 10, H, KP), bf16),
            V((3, KP, C), bf16),
            V((3, C, KP), bf16),
            V((B, W, H, CP), f32),
            V((B, W, H, CP), f32),
            V((B, CP, W * H), bf16),
            V((T, C, HALF), f32),
            V((T, X, Y, ZL, RB, 8, CH), f32),
            V((T, Y, RB, 8, CH), f32),
            V((T, X, RB, 8, CH), f32),
            V((T, 40, 8, HALF), bf16),
            V((T, 40, 8, HALF), bf16),
            V((T, X, Y, ZL, RB, 8, CH), bf16),
            V((T, X - 1, Y, RB, 8, CH), bf16),
            V((T, Y - 1, X, RB, 8, CH), bf16),
            V((T, Y, RB, 8, CH), bf16),
            V((T, X, RB, 8, CH), bf16),
            V((T, Y - 1, RB, 8, CH), bf16),
            V((T, X - 1, RB, 8, CH), bf16),
            V((T, ZL, RB, 8, CH), bf16),
            V((T, NZ, RB, 8, CH), bf16),
            V((T, NP, RB, 8, CH), bf16),
            V((B, W, H, CP), f32),
            V((NA, 1, 128), f32),
            V((NB, 1, 128), f32),
            V((NA, 1, 128), f32),
            V((NB, 1, 128), f32),
            V((NA, B, CP), f32),
            V((NB, B, CP), f32),
            V((NA, B, CP), f32),
            V((NB, B, CP), f32),
            D((11,)),
            D((2, 8)),
            D((2, 8)),
            D((8,)),
            D((8,)),
            D((T,)),
            D((T,)),
            D((T,)),
            D((T,)),
            D((T,)),
            D((T,)),
            D((T,)),
            D((T,)),
            D((T,)),
            D((T,)),
            D((T,)),
            D((T,)),
            D((T,)),
            D((T,)),
        ],
        compiler_params=pltpu.CompilerParams(collective_id=0, has_side_effects=True, vmem_limit_bytes=LIMIT),
        name="block",
    )(timestep, gain, bias, conv_b, latent, cotangent, conv_w, embed_in, embed_out, time_w.T)
    bo, ig, cwg, twg, gg, bg, cbg = pl.pallas_call(
        write_out,
        out_shape=(
            jax.ShapeDtypeStruct((B, H, W, C), bf16),
            jax.ShapeDtypeStruct((B, H, W, C), f32),
            jax.ShapeDtypeStruct((3, 3, RB * 8, C), f32),
            jax.ShapeDtypeStruct((C, TE), f32),
            jax.ShapeDtypeStruct((C,), f32),
            jax.ShapeDtypeStruct((C,), f32),
            jax.ShapeDtypeStruct((C,), f32),
        ),
        in_specs=[vmem] * 5,
        out_specs=(anyspace,) * 4 + (vmem,) * 3,
        scratch_shapes=[D((4,))],
        compiler_params=pltpu.CompilerParams(vmem_limit_bytes=1024 * 1024),
        name="write_out",
    )(*held)
    return bo, ig, cwg.transpose(2, 0, 1, 3), gg, bg, cbg, twg.T


def build(finer):
    sizes = tuple(finer.shape[a] for a in AXES)
    image = P(None, ROW, COL, None)
    return jax.shard_map(
        functools.partial(step, sizes),
        mesh=finer,
        in_specs=(image, P(), P(), P(), P(), P(), P(), P(), P(), image),
        out_specs=(image, image, P(ROW, None, None, None), P(), P(), P(), P()),
        check_vma=False,
    )


def solution(mesh):
    return build(Mesh(mesh.devices.reshape(4, 2, 4, 4, 2), AXES))
```
